16 devices in a mesh: replica: 2 (over z), data: 8 (over y, x, core).
Axes of the slice: x: 2, y: 2, z: 2, core: 2. Of those that a mesh axis runs over, the one named last changes fastest.
Arguments:
- x: bfloat16 [8192, 3072], P(('replica', 'data')), parts along dimension 0
- adapter_id: int32 [8192], P(('replica', 'data')), parts along dimension 0
- w_gate: bfloat16 [3072, 8192], replicated
- w_up: bfloat16 [3072, 8192], replicated
- w_down: bfloat16 [8192, 3072], replicated
- a_gate: bfloat16 [64, 3072, 64], P('data')
- b_gate: bfloat16 [64, 64, 8192], P('data')
- a_up: bfloat16 [64, 3072, 64], P('data')
- b_up: bfloat16 [64, 64, 8192], P('data')
- a_down: bfloat16 [64, 8192, 64], P('data')
- b_down: bfloat16 [64, 64, 3072], P('data')
- hot_ids: int32 [4], replicated
- hot_a_gate: bfloat16 [4, 3072, 64], replicated
- hot_b_gate: bfloat16 [4, 64, 8192], replicated
- hot_a_up: bfloat16 [4, 3072, 64], replicated
- hot_b_up: bfloat16 [4, 64, 8192], replicated
- hot_a_down: bfloat16 [4, 8192, 64], replicated
- hot_b_down: bfloat16 [4, 64, 3072], replicated
Outputs:
- output: bfloat16 [8192, 3072], P(('replica', 'data')), parts along dimension 0
There are 2 independent parts. The reference program is written for one: setup_inputs(seed, part) draws one part's arguments, and reference() takes and returns one part's arrays. A program takes and returns all parts, laid end to end along the dimension named above; an argument that names none is the same for every part.
All inputs are finite; a program needn't handle non-finite values.
Results may differ from the reference program's by a relative error of at most 0.00144.
Values are sent between devices in bfloat16 or wider.
A program may use at most 1 GiB of HBM per device.

```python
import jax
import jax.numpy as jnp
from jax import lax

GROUP = 8
T_LOC = 512
D = 3072
F = 8192
R = 64
N_LOC = 8
HOT_K = 4
LORA_ALPHA = 32
TOK_BLOCK = 128
TOKENS = GROUP * T_LOC
ADAPTERS = GROUP * N_LOC
CAP = T_LOC // (2 * GROUP)
LORA_SCALE = LORA_ALPHA / R


def draw_hot(hot_key):
    owner_key, local_key = jax.random.split(hot_key)
    hot_owner = jax.random.permutation(owner_key, GROUP)[:HOT_K]
    hot_local = jax.random.randint(local_key, (HOT_K,), 0, N_LOC)
    return hot_owner, hot_local


def draw_ids(id_key, hot_owner, hot_local):
    shift_key, peak_key, count_key, perm_key, cold_key, pick_key = jax.random.split(id_key, 6)
    owners = jnp.arange(GROUP)
    peak_owner = jax.random.randint(peak_key, (), 0, GROUP)
    pop_shift = jnp.where(owners == peak_owner, 0, jax.random.randint(shift_key, (GROUP,), 0, 4))
    cap_upper = jnp.maximum(CAP // (2 ** pop_shift), 1)
    cap_lower = jnp.maximum(cap_upper // 2, 1)
    counts = jax.random.randint(count_key, (GROUP, GROUP), cap_lower[None, :], cap_upper[None, :] + 1)
    counts = jnp.where(owners[None, :] == peak_owner, CAP, counts)
    count_ends = jnp.cumsum(counts, axis=1)
    positions = jnp.arange(T_LOC)

    def owner_row(end_row):
        return jnp.searchsorted(end_row, positions, side='right')

    owner_seq = jax.vmap(owner_row)(count_ends)
    owner_seq = jax.random.permutation(perm_key, owner_seq, axis=1, independent=True)
    owner_safe = jnp.minimum(owner_seq, GROUP - 1)
    hot_match = hot_owner[None, :] == owners[:, None]
    has_hot = jnp.any(hot_match, axis=1).astype(jnp.int32)
    skip_local = jnp.sum(jnp.where(hot_match, hot_local[None, :], 0), axis=1) + (1 - has_hot) * N_LOC
    pick_local = jax.random.randint(cold_key, (GROUP, T_LOC), 0, N_LOC - has_hot[owner_safe])
    pick_local = pick_local + (pick_local >= skip_local[owner_safe]).astype(jnp.int32)
    cold_ids = owner_safe * N_LOC + pick_local
    hot_list = hot_owner * N_LOC + hot_local
    hot_tok = hot_list[jax.random.randint(pick_key, (GROUP, T_LOC), 0, HOT_K)]
    tok_ids = jnp.where(owner_seq == GROUP, hot_tok, cold_ids)
    return tok_ids.reshape(TOKENS).astype(jnp.int32)


def normal_weights(w_key, shape, std):
    return (jax.random.normal(w_key, shape, jnp.float32) * std).astype(jnp.bfloat16)


def adapter_set(set_key, adapter_count):
    set_keys = jax.random.split(set_key, 6)
    b_std = 0.5 / (LORA_SCALE * R ** 0.5)
    return [
        normal_weights(set_keys[0], (adapter_count, D, R), D ** -0.5),
        normal_weights(set_keys[1], (adapter_count, R, F), b_std),
        normal_weights(set_keys[2], (adapter_count, D, R), D ** -0.5),
        normal_weights(set_keys[3], (adapter_count, R, F), b_std),
        normal_weights(set_keys[4], (adapter_count, F, R), F ** -0.5),
        normal_weights(set_keys[5], (adapter_count, R, D), b_std),
    ]


def setup_inputs(seed: int = 0, part: int = 0) -> dict:
    root_key = jax.random.key(seed)
    base_keys = jax.random.split(jax.random.fold_in(root_key, 1), 3)
    route_key = jax.random.fold_in(root_key, 3)
    hot_owner, hot_local = draw_hot(jax.random.fold_in(route_key, 2))
    tok_ids = draw_ids(jax.random.fold_in(jax.random.fold_in(route_key, 1), part), hot_owner, hot_local)
    x_key = jax.random.fold_in(jax.random.fold_in(root_key, 5), part)
    store_set = adapter_set(jax.random.fold_in(root_key, 2), ADAPTERS)
    hot_set = adapter_set(jax.random.fold_in(root_key, 4), HOT_K)
    return {
        'x': jax.random.normal(x_key, (TOKENS, D), jnp.float32).astype(jnp.bfloat16),
        'adapter_id': tok_ids,
        'w_gate': normal_weights(base_keys[0], (D, F), D ** -0.5),
        'w_up': normal_weights(base_keys[1], (D, F), D ** -0.5),
        'w_down': normal_weights(base_keys[2], (F, D), F ** -0.5),
        'a_gate': store_set[0],
        'b_gate': store_set[1],
        'a_up': store_set[2],
        'b_up': store_set[3],
        'a_down': store_set[4],
        'b_down': store_set[5],
        'hot_ids': (hot_owner * N_LOC + hot_local).astype(jnp.int32),
        'hot_a_gate': hot_set[0],
        'hot_b_gate': hot_set[1],
        'hot_a_up': hot_set[2],
        'hot_b_up': hot_set[3],
        'hot_a_down': hot_set[4],
        'hot_b_down': hot_set[5],
    }


def lora_delta(tok_rows, a_rows, b_rows):
    low_rank = jnp.einsum('td,tdr->tr', tok_rows.astype(jnp.float32), a_rows.astype(jnp.float32)).astype(jnp.bfloat16)
    delta_f = jnp.einsum('tr,trf->tf', low_rank.astype(jnp.float32), b_rows.astype(jnp.float32))
    return (LORA_SCALE * delta_f).astype(jnp.bfloat16)


def reference(x, adapter_id, w_gate, w_up, w_down, a_gate, b_gate, a_up, b_up, a_down, b_down, hot_ids, hot_a_gate, hot_b_gate, hot_a_up, hot_b_up, hot_a_down, hot_b_down):
    def block_out(block_args):
        tok_rows, tok_ids = block_args
        hot_match = tok_ids[:, None] == hot_ids[None, :]
        is_hot = jnp.any(hot_match, axis=1)
        hot_slot = jnp.sum(jnp.where(hot_match, jnp.arange(HOT_K)[None, :], 0), axis=1)

        def chosen(store_set, hot_copy):
            return jnp.where(is_hot[:, None, None], hot_copy[hot_slot], store_set[tok_ids])

        gate_act = jnp.dot(tok_rows, w_gate, preferred_element_type=jnp.float32) + lora_delta(tok_rows, chosen(a_gate, hot_a_gate), chosen(b_gate, hot_b_gate)).astype(jnp.float32)
        up_act = jnp.dot(tok_rows, w_up, preferred_element_type=jnp.float32) + lora_delta(tok_rows, chosen(a_up, hot_a_up), chosen(b_up, hot_b_up)).astype(jnp.float32)
        hidden = (jax.nn.silu(gate_act) * up_act).astype(jnp.bfloat16)
        down_out = jnp.dot(hidden, w_down, preferred_element_type=jnp.float32) + lora_delta(hidden, chosen(a_down, hot_a_down), chosen(b_down, hot_b_down)).astype(jnp.float32)
        return (tok_rows.astype(jnp.float32) + down_out).astype(jnp.bfloat16)

    blocks = lax.map(block_out, (x.reshape(TOKENS // TOK_BLOCK, TOK_BLOCK, D), adapter_id.reshape(TOKENS // TOK_BLOCK, TOK_BLOCK)))
    return blocks.reshape(TOKENS, D)
```

```python
import functools

import jax
import jax.numpy as jnp
from jax import lax
from jax.experimental import pallas as pl
from jax.experimental.pallas import tpu as pltpu
from jax.sharding import PartitionSpec as P

LORA_ALPHA = 32
MESH = pl.DeviceIdType.MESH
F32 = jnp.float32
BF16 = jnp.bfloat16

TN = 512
FIRST = 8


def dot(a, b):
    return jnp.dot(a, b, preferred_element_type=F32)


def dot_t(a, b):
    return lax.dot_general(a, b, (((1,), (1,)), ((), ())), preferred_element_type=F32)


def positions(ids, hot_ids, n_hot, group, n_local, cap):
    tokens = ids.shape[1]
    kept = tokens - group * cap
    is_hot = ids < 0
    hot_idx = jnp.zeros_like(ids)
    for j in range(n_hot):
        match = ids == hot_ids[j]
        is_hot = is_hot | match
        hot_idx = jnp.where(match, j, hot_idx)
    owner = jnp.where(is_hot, group, ids // n_local)
    local = ids - (ids // n_local) * n_local
    cls = jnp.where(is_hot, n_local + hot_idx, local)
    rows = 2 * group
    kind = lax.broadcasted_iota(jnp.int32, (rows, tokens), 0)
    member = (kind == jnp.broadcast_to(owner, (rows, tokens))).astype(F32)
    before = lax.broadcasted_iota(jnp.int32, (tokens, tokens), 0) < lax.broadcasted_iota(jnp.int32, (tokens, tokens), 1)
    cum = dot(member.astype(BF16), before.astype(BF16))
    rank = jnp.sum(member * cum, axis=0, keepdims=True)
    counts = jnp.sum(member, axis=1, keepdims=True)
    sub = lax.broadcasted_iota(jnp.int32, (rows, 1), 0)
    holes = jnp.where(sub < group, cap - counts, 0.0)
    lower = lax.broadcasted_iota(jnp.int32, (rows, rows), 1) < lax.broadcasted_iota(jnp.int32, (rows, rows), 0)
    hole_start = dot(lower.astype(BF16), jnp.broadcast_to(holes, (rows, 128)).astype(BF16))[:, 0:1]
    spill = jnp.broadcast_to(rank - kept, (rows, tokens))
    takes = (spill >= hole_start) & (spill < hole_start + holes)
    base = kept + cap * sub.astype(F32) + counts - hole_start
    filled = jnp.sum(jnp.where(takes, base + spill, 0.0), axis=0, keepdims=True)
    own = kept + cap * owner.astype(F32) + rank
    pos = jnp.where(is_hot, jnp.where(rank < kept, rank, filled), own)
    return pos, cls.astype(F32)


def masked(low, cls, first_group, rank):
    per = 128 // rank
    lane = lax.broadcasted_iota(jnp.int32, (low.shape[0], 128), 1) // rank
    parts = []
    for k in range(low.shape[1] // 128):
        here = (lane + per * (first_group + k)).astype(F32) == cls
        parts.append(jnp.where(here, low[:, k * 128:(k + 1) * 128], 0.0).astype(BF16))
    return jnp.concatenate(parts, axis=1)


def mlp_kernel(group, n_local, n_hot, rank, scale,
               hot_ids, ids, x_hbm, wg_hbm, wu_hbm, wd_hbm,
               ag_hbm, bg_hbm, au_hbm, bu_hbm, ad_hbm, bd_hbm,
               hag_hbm, hbg_hbm, hau_hbm, hbu_hbm, had_hbm, hbd_hbm,
               out_hbm,
               x_v, xsend, xa, h, pg, pu, pd, pdm, at, wbuf, bbuf, adbuf, y_send, y_back, y_kept, o_stage, unperm,
               x_sem, at_sem, w_sem, o_sem, s1, r1, s2, r2):
    me = lax.axis_index("data")
    tokens, d_model = x_hbm.shape
    d_ff = wg_hbm.shape[1]
    cap = tokens // (2 * group)
    half = group * cap
    n_own = n_local * rank
    n_hr = n_hot * rank
    n_all = n_own + n_hr
    n_tiles = d_ff // TN
    d_tiles = d_model // TN
    k_half = d_ff // 2
    kept = pl.ds(0, half)
    recv = pl.ds(half, half)
    hot_cols = pl.ds(n_own, n_hr)
    hot_group = n_own // 128

    def cp(src, dst, sem):
        return pltpu.make_async_copy(src, dst, sem)

    def gu_copies(tile, slot, full):
        cols = pl.ds(pl.multiple_of(tile * TN, TN), TN)
        out = [
            cp(wg_hbm.at[:, cols], wbuf.at[slot, 0, pl.ds(0, d_model)], w_sem.at[slot, 0]),
            cp(wu_hbm.at[:, cols], wbuf.at[slot, 1, pl.ds(0, d_model)], w_sem.at[slot, 1]),
            cp(hbg_hbm.at[:, cols], bbuf.at[slot, 0, hot_cols], w_sem.at[slot, 2]),
            cp(hbu_hbm.at[:, cols], bbuf.at[slot, 1, hot_cols], w_sem.at[slot, 3]),
        ]
        if full:
            out += [
                cp(bg_hbm.at[:, cols], bbuf.at[slot, 0, pl.ds(0, n_own)], w_sem.at[slot, 4]),
                cp(bu_hbm.at[:, cols], bbuf.at[slot, 1, pl.ds(0, n_own)], w_sem.at[slot, 5]),
                cp(ad_hbm.at[:, cols], adbuf.at[slot, pl.ds(0, n_own)], w_sem.at[slot, 6]),
                cp(had_hbm.at[:, cols], adbuf.at[slot, hot_cols], w_sem.at[slot, 7]),
            ]
        return out

    def down_copies(tile, slot):
        cols = pl.ds(pl.multiple_of(tile * TN, TN), TN)
        return [
            cp(wd_hbm.at[pl.ds(0, k_half), cols], wbuf.at[slot, 0], w_sem.at[slot, 0]),
            cp(wd_hbm.at[pl.ds(k_half, k_half), cols], wbuf.at[slot, 1], w_sem.at[slot, 1]),
            cp(bd_hbm.at[:, cols], bbuf.at[slot, 0, pl.ds(0, n_own)], w_sem.at[slot, 4]),
            cp(hbd_hbm.at[:, cols], bbuf.at[slot, 0, hot_cols], w_sem.at[slot, 2]),
        ]

    def start(copies):
        for c in copies:
            c.start()

    def wait(copies):
        for c in copies:
            c.wait()

    x_copy = cp(x_hbm, x_v, x_sem)
    x_copy.start()
    at_hot = [cp(hag_hbm, at.at[0, hot_cols], at_sem.at[0]), cp(hau_hbm, at.at[1, hot_cols], at_sem.at[1])]
    at_own = [cp(ag_hbm, at.at[0, pl.ds(0, n_own)], at_sem.at[2]), cp(au_hbm, at.at[1, pl.ds(0, n_own)], at_sem.at[3])]
    start(at_hot)
    start(gu_copies(0, 0, False))
    start(at_own)

    barrier = pltpu.get_barrier_semaphore()
    for d in range(1, group):
        pl.semaphore_signal(barrier, inc=1, device_id={"data": lax.rem(me + d, group)}, device_id_type=MESH)

    pos, cls = positions(ids[...], hot_ids, n_hot, group, n_local, cap)
    place = jnp.broadcast_to(pos.astype(jnp.int32), (tokens, tokens))
    perm = (place == lax.broadcasted_iota(jnp.int32, (tokens, tokens), 0)).astype(BF16)
    cls_rows = dot_t(perm, jnp.broadcast_to(cls, (128, tokens)).astype(BF16)).astype(BF16)
    pos_col = jnp.transpose(jnp.broadcast_to(pos, (128, tokens)))[:, 0:1].astype(jnp.int32)
    unperm[...] = (pos_col == lax.broadcasted_iota(jnp.int32, (tokens, tokens), 1)).astype(BF16)
    xsend[:, pl.ds(d_model, 128)] = cls_rows[half:]
    xa[kept, pl.ds(d_model, 128)] = cls_rows[:half]
    x_copy.wait()
    for n in range(d_tiles):
        cols = pl.ds(n * TN, TN)
        moved = dot(perm, x_v[:, cols])
        xsend[:, cols] = moved[half:].astype(BF16)
        xa[kept, cols] = moved[:half].astype(BF16)

    pl.semaphore_wait(barrier, group - 1)
    my_block = pl.ds(pl.multiple_of(me * cap, cap), cap)
    my_rows = pl.ds(pl.multiple_of(half + me * cap, cap), cap)

    def x_remote(d):
        to = lax.rem(me + d, group)
        return pltpu.make_async_remote_copy(
            src_ref=xsend.at[pl.ds(pl.multiple_of(to * cap, cap), cap)], dst_ref=xa.at[my_rows],
            send_sem=s1.at[d], recv_sem=r1.at[d], device_id={"data": to}, device_id_type=MESH)

    for d in range(1, group):
        x_remote(d).start()
    xa[my_rows, :] = xsend[my_block, :]

    def lora(low, b):
        return (scale * dot(low, b)).astype(BF16).astype(F32)

    def act(g, u):
        return (g * jax.nn.sigmoid(g) * u).astype(BF16)

    cls_kept = xa[kept, pl.ds(d_model, 128)].astype(F32)
    for i, p in ((0, pg), (1, pu)):
        at_hot[i].wait()
        low = dot_t(xa[kept, pl.ds(0, d_model)], at[i, hot_cols, :])
        p[kept, hot_cols] = masked(low.astype(BF16).astype(F32), cls_kept, hot_group, rank)

    def first_step(s, carry):
        slot = lax.rem(s, 2)

        @pl.when(s + 1 < FIRST)
        def _():
            start(gu_copies(s + 1, 1 - slot, False))

        @pl.when(s + 1 == FIRST)
        def _():
            start(gu_copies(0, 1 - slot, True))

        wait(gu_copies(s, slot, False))
        xk = xa[kept, pl.ds(0, d_model)]
        g = dot(xk, wbuf[slot, 0, pl.ds(0, d_model), :]) + lora(pg[kept, hot_cols], bbuf[slot, 0, hot_cols, :])
        u = dot(xk, wbuf[slot, 1, pl.ds(0, d_model), :]) + lora(pu[kept, hot_cols], bbuf[slot, 1, hot_cols, :])
        h[kept, pl.ds(pl.multiple_of(s * TN, TN), TN)] = act(g, u)
        return carry

    lax.fori_loop(0, FIRST, first_step, 0)

    for d in range(1, group):
        x_remote(d).wait_recv()
    cls_recv = xa[recv, pl.ds(d_model, 128)].astype(F32)
    for i, p in ((0, pg), (1, pu)):
        at_own[i].wait()
        low = dot_t(xa[recv, pl.ds(0, d_model)], at[i])
        p[recv, :] = masked(low.astype(BF16).astype(F32), cls_recv, 0, rank)
    pd[...] = jnp.zeros_like(pd)

    def add_low(slot, cols):
        pd[kept, hot_cols] += dot_t(h[kept, cols], adbuf[slot, hot_cols, :])
        pd[recv, :] += dot_t(h[recv, cols], adbuf[slot])

    def second_step(s, carry):
        slot = lax.rem(s + FIRST, 2)
        start(gu_copies(s + 1, 1 - slot, True))
        wait(gu_copies(s, slot, True))
        cols = pl.ds(pl.multiple_of(s * TN, TN), TN)
        xr = xa[recv, pl.ds(0, d_model)]
        g = dot(xr, wbuf[slot, 0, pl.ds(0, d_model), :]) + lora(pg[recv, :], bbuf[slot, 0])
        u = dot(xr, wbuf[slot, 1, pl.ds(0, d_model), :]) + lora(pu[recv, :], bbuf[slot, 1])
        h[recv, cols] = act(g, u)
        add_low(slot, cols)
        return carry

    lax.fori_loop(0, FIRST, second_step, 0)

    def both_lora(p, slot, i, n_rows=None):
        return lora(p[kept, hot_cols], bbuf[slot, i, hot_cols, :]), lora(p[recv, :], bbuf[slot, i])

    def third_step(s, carry):
        slot = lax.rem(s + FIRST, 2)

        @pl.when(s + 1 < n_tiles)
        def _():
            start(gu_copies(s + 1, 1 - slot, True))

        @pl.when(s + 1 == n_tiles)
        def _():
            start(down_copies(0, 1 - slot))

        wait(gu_copies(s, slot, True))
        cols = pl.ds(pl.multiple_of(s * TN, TN), TN)
        xx = xa[:, pl.ds(0, d_model)]
        g = dot(xx, wbuf[slot, 0, pl.ds(0, d_model), :])
        u = dot(xx, wbuf[slot, 1, pl.ds(0, d_model), :])
        gk, gr = both_lora(pg, slot, 0)
        uk, ur = both_lora(pu, slot, 1)
        h[kept, cols] = act(g[:half] + gk, u[:half] + uk)
        h[recv, cols] = act(g[half:] + gr, u[half:] + ur)
        add_low(slot, cols)
        return carry

    lax.fori_loop(FIRST, n_tiles, third_step, 0)
    slot0 = (n_tiles + FIRST) % 2

    pdm[kept, hot_cols] = masked(pd[kept, hot_cols].astype(BF16).astype(F32), cls_kept, hot_group, rank)
    pdm[recv, :] = masked(pd[recv, :].astype(BF16).astype(F32), cls_recv, 0, rank)

    def y_remote(n, d):
        to = lax.rem(me + d, group)
        return pltpu.make_async_remote_copy(
            src_ref=y_send.at[n, pl.ds(pl.multiple_of(to * cap, cap), cap)], dst_ref=y_back.at[n, my_block],
            send_sem=s2.at[n, d], recv_sem=r2.at[n, d], device_id={"data": to}, device_id_type=MESH)

    def rows_out(n, slot, rows, low):
        cols = pl.ds(pl.multiple_of(n * TN, TN), TN)
        y = dot(h[rows, pl.ds(0, k_half)], wbuf[slot, 0]) + dot(h[rows, pl.ds(k_half, k_half)], wbuf[slot, 1])
        return (xa[rows, cols].astype(F32) + (y + low)).astype(BF16)

    def down_recv(n, slot):
        y_send[n] = rows_out(n, slot, recv, lora(pdm[recv, :], bbuf[slot, 0]))

    def down_kept(n, slot):
        y_kept[n] = rows_out(n, slot, kept, lora(pdm[kept, hot_cols], bbuf[slot, 0, hot_cols, :]))

    def send_back(n):
        for d in range(1, group):
            y_remote(n, d).start()
        y_back[n, my_block, :] = y_send[n, my_block, :]

    def out_copy(n, slot):
        return cp(o_stage.at[slot], out_hbm.at[:, pl.ds(pl.multiple_of(n * TN, TN), TN)], o_sem.at[slot])

    def finish(n, slot):
        for d in range(1, group):
            y_remote(n, d).wait_recv()
        o_stage[slot] = (dot(unperm[:, pl.ds(0, half)], y_kept[n]) + dot(unperm[:, pl.ds(half, half)], y_back[n])).astype(BF16)
        out_copy(n, slot).start()

    def down_step(n, carry):
        slot = lax.rem(n + slot0, 2)

        @pl.when(n + 1 < d_tiles)
        def _():
            start(down_copies(n + 1, 1 - slot))

        wait(down_copies(n, slot))
        down_recv(n, slot)
        send_back(n)
        down_kept(n, slot)

        @pl.when(n > 0)
        def _():
            @pl.when(n > 2)
            def _():
                out_copy(n - 3, lax.rem(n + 1, 2)).wait()
            finish(n - 1, lax.rem(n + 1, 2))
        return carry

    lax.fori_loop(0, d_tiles, down_step, 0)
    last = d_tiles - 1
    out_copy(last - 2, last % 2).wait()
    finish(last, last % 2)
    out_copy(last - 1, 1 - last % 2).wait()
    out_copy(last, last % 2).wait()

    for d in range(1, group):
        x_remote(d).wait_send()

    def drain(n, carry):
        for d in range(1, group):
            y_remote(n, d).wait_send()
        return carry

    lax.fori_loop(0, d_tiles, drain, 0)


def solution(mesh):
    group = mesh.shape["data"]
    token_spec = P(("replica", "data"), None)
    store_spec = P("data", None, None)
    full_mat = P(None, None)
    full_set = P(None, None, None)
    in_specs = (token_spec, P(("replica", "data")), full_mat, full_mat, full_mat) + (store_spec,) * 6 + (P(None),) + (full_set,) * 6

    def device_step(x, adapter_id, w_gate, w_up, w_down, a_gate, b_gate, a_up, b_up, a_down, b_down, hot_ids, hot_a_gate, hot_b_gate, hot_a_up, hot_b_up, hot_a_down, hot_b_down):
        tokens, d_model = x.shape
        d_ff = w_gate.shape[1]
        n_local, _, rank = a_gate.shape
        n_hot = hot_ids.shape[0]
        cap = tokens // (2 * group)
        half = group * cap
        n_all = (n_local + n_hot) * rank
        d_tiles = d_model // TN

        def a_t(a):
            return jnp.swapaxes(a, 1, 2).reshape(a.shape[0] * rank, a.shape[1])

        def b_flat(b):
            return b.reshape(b.shape[0] * rank, b.shape[2])

        hbm = pl.BlockSpec(memory_space=pl.ANY)
        kernel = functools.partial(mlp_kernel, group, n_local, n_hot, rank, LORA_ALPHA / rank)
        return pl.pallas_call(
            kernel,
            out_shape=jax.ShapeDtypeStruct(x.shape, x.dtype),
            in_specs=[pl.BlockSpec(memory_space=pltpu.SMEM), pl.BlockSpec(memory_space=pltpu.VMEM)] + [hbm] * 16,
            out_specs=hbm,
            scratch_shapes=[
                pltpu.VMEM((tokens, d_model), BF16),
                pltpu.VMEM((half, d_model + 128), BF16),
                pltpu.VMEM((tokens, d_model + 128), BF16),
                pltpu.VMEM((tokens, d_ff), BF16),
                pltpu.VMEM((tokens, n_all), BF16),
                pltpu.VMEM((tokens, n_all), BF16),
                pltpu.VMEM((tokens, n_all), F32),
                pltpu.VMEM((tokens, n_all), BF16),
                pltpu.VMEM((2, n_all, d_model), BF16),
                pltpu.VMEM((2, 2, d_ff // 2, TN), BF16),
                pltpu.VMEM((2, 2, n_all, TN), BF16),
                pltpu.VMEM((2, n_all, TN), BF16),
                pltpu.VMEM((d_tiles, half, TN), BF16),
                pltpu.VMEM((d_tiles, half, TN), BF16),
                pltpu.VMEM((d_tiles, half, TN), BF16),
                pltpu.VMEM((2, tokens, TN), BF16),
                pltpu.VMEM((tokens, tokens), BF16),
                pltpu.SemaphoreType.DMA,
                pltpu.SemaphoreType.DMA((4,)),
                pltpu.SemaphoreType.DMA((2, 8)),
                pltpu.SemaphoreType.DMA((2,)),
                pltpu.SemaphoreType.DMA((group,)),
                pltpu.SemaphoreType.DMA((group,)),
                pltpu.SemaphoreType.DMA((d_tiles, group)),
                pltpu.SemaphoreType.DMA((d_tiles, group)),
            ],
            compiler_params=pltpu.CompilerParams(
                collective_id=0, has_side_effects=True, vmem_limit_bytes=67043328),
        )(hot_ids, adapter_id.reshape(1, tokens), x, w_gate, w_up, w_down,
          a_t(a_gate), b_flat(b_gate), a_t(a_up), b_flat(b_up), a_t(a_down), b_flat(b_down),
          a_t(hot_a_gate), b_flat(hot_b_gate), a_t(hot_a_up), b_flat(hot_b_up), a_t(hot_a_down), b_flat(hot_b_down))

    return jax.shard_map(device_step, mesh=mesh, in_specs=in_specs, out_specs=token_spec, check_vma=False)
```

```python
import functools

import jax
import jax.numpy as jnp
from jax import lax
from jax.experimental import pallas as pl
from jax.experimental.pallas import tpu as pltpu
from jax.sharding import PartitionSpec as P

LORA_ALPHA = 32
MESH = pl.DeviceIdType.MESH
F32 = jnp.float32
BF16 = jnp.bfloat16

TN = 512
FIRST = 8


def dot(a, b):
    return jnp.dot(a, b, preferred_element_type=F32)


def dot_t(a, b):
    return lax.dot_general(a, b, (((1,), (1,)), ((), ())), preferred_element_type=F32)


def positions(ids, hot_ids, n_hot, group, n_local, cap):
    tokens = ids.shape[1]
    kept = tokens - group * cap
    is_hot = ids < 0
    hot_idx = jnp.zeros_like(ids)
    for j in range(n_hot):
        match = ids == hot_ids[j]
        is_hot = is_hot | match
        hot_idx = jnp.where(match, j, hot_idx)
    owner = jnp.where(is_hot, group, ids // n_local)
    local = ids - (ids // n_local) * n_local
    cls = jnp.where(is_hot, n_local + hot_idx, local)
    rows = 2 * group
    kind = lax.broadcasted_iota(jnp.int32, (rows, tokens), 0)
    member = (kind == jnp.broadcast_to(owner, (rows, tokens))).astype(F32)
    before = lax.broadcasted_iota(jnp.int32, (tokens, tokens), 0) < lax.broadcasted_iota(jnp.int32, (tokens, tokens), 1)
    cum = dot(member.astype(BF16), before.astype(BF16))
    rank = jnp.sum(member * cum, axis=0, keepdims=True)
    counts = jnp.sum(member, axis=1, keepdims=True)
    sub = lax.broadcasted_iota(jnp.int32, (rows, 1), 0)
    holes = jnp.where(sub < group, cap - counts, 0.0)
    lower = lax.broadcasted_iota(jnp.int32, (rows, rows), 1) < lax.broadcasted_iota(jnp.int32, (rows, rows), 0)
    hole_start = dot(lower.astype(BF16), jnp.broadcast_to(holes, (rows, 128)).astype(BF16))[:, 0:1]
    spill = jnp.broadcast_to(rank - kept, (rows, tokens))
    takes = (spill >= hole_start) & (spill < hole_start + holes)
    base = kept + cap * sub.astype(F32) + counts - hole_start
    filled = jnp.sum(jnp.where(takes, base + spill, 0.0), axis=0, keepdims=True)
    own = kept + cap * owner.astype(F32) + rank
    pos = jnp.where(is_hot, jnp.where(rank < kept, rank, filled), own)
    return pos, cls.astype(F32)


def masked(low, cls, first_group, rank):
    per = 128 // rank
    lane = lax.broadcasted_iota(jnp.int32, (low.shape[0], 128), 1) // rank
    parts = []
    for k in range(low.shape[1] // 128):
        here = (lane + per * (first_group + k)).astype(F32) == cls
        parts.append(jnp.where(here, low[:, k * 128:(k + 1) * 128], 0.0).astype(BF16))
    return jnp.concatenate(parts, axis=1)


def mlp_kernel(group, n_local, n_hot, rank, scale,
               hot_hbm, ids_hbm, x_hbm, wg_hbm, wu_hbm, wd_hbm,
               ag_hbm, bg_hbm, au_hbm, bu_hbm, ad_hbm, bd_hbm,
               hag_hbm, hbg_hbm, hau_hbm, hbu_hbm, had_hbm, hbd_hbm,
               out_hbm,
               hot_ids, ids, xy, xsend, xa, h, pg, pu, pd, pdm, at, wbuf, bbuf, adbuf, y_kept, o_stage, unperm,
               id_sem, x_sem, at_sem, w_sem, d_sem, o_sem, s1, r1, s2, r2):
    me = lax.axis_index("data")
    tokens, d_model = x_hbm.shape
    d_ff = wg_hbm.shape[1]
    cap = tokens // (2 * group)
    half = group * cap
    n_own = n_local * rank
    n_hr = n_hot * rank
    n_tiles = d_ff // TN
    d_tiles = d_model // TN
    kept = pl.ds(0, half)
    recv = pl.ds(half, half)
    own_cols = pl.ds(0, n_own)
    hot_cols = pl.ds(n_own, n_hr)
    hot_group = n_own // 128
    steps = FIRST + n_tiles
    lead = steps % 3
    k_parts = [(k, min(d_model, d_ff - k)) for k in range(0, d_ff, d_model)]
    assert len(k_parts) == 3

    def cp(src, dst, sem):
        return pltpu.make_async_copy(src, dst, sem)

    def tile_cols(tile):
        return pl.ds(tile * TN if isinstance(tile, int) else pl.multiple_of(tile * TN, TN), TN)

    def gu_copies(tile, slot, full):
        cols = tile_cols(tile)
        out = [
            cp(wg_hbm.at[:, cols], wbuf.at[2 * slot], w_sem.at[slot, 0]),
            cp(wu_hbm.at[:, cols], wbuf.at[2 * slot + 1], w_sem.at[slot, 1]),
            cp(hbg_hbm.at[:, cols], bbuf.at[slot, 0, hot_cols], w_sem.at[slot, 2]),
            cp(hbu_hbm.at[:, cols], bbuf.at[slot, 1, hot_cols], w_sem.at[slot, 3]),
        ]
        if full:
            out += [
                cp(bg_hbm.at[:, cols], bbuf.at[slot, 0, own_cols], w_sem.at[slot, 4]),
                cp(bu_hbm.at[:, cols], bbuf.at[slot, 1, own_cols], w_sem.at[slot, 5]),
                cp(ad_hbm.at[:, cols], adbuf.at[slot, own_cols], w_sem.at[slot, 6]),
                cp(had_hbm.at[:, cols], adbuf.at[slot, hot_cols], w_sem.at[slot, 7]),
            ]
        return out

    def down_half(n, i):
        return lax.rem(2 * lead + 3 * lax.rem(n, 2) + i, 6)

    def down_b(n):
        return lax.rem(lead + lax.rem(n, 2), 3)

    def down_copies(n, pieces=(0, 1, 2, 3, 4)):
        cols = tile_cols(n)
        side = lax.rem(n, 2)
        out = []
        for i in pieces:
            if i < 3:
                k, size = k_parts[i]
                src, dst = wd_hbm.at[pl.ds(k, size), cols], wbuf.at[down_half(n, i), pl.ds(0, size)]
            elif i == 3:
                src, dst = bd_hbm.at[:, cols], bbuf.at[down_b(n), 0, own_cols]
            else:
                src, dst = hbd_hbm.at[:, cols], bbuf.at[down_b(n), 0, hot_cols]
            out.append(cp(src, dst, d_sem.at[side, i]))
        return out

    def start(copies):
        for c in copies:
            c.start()

    def wait(copies):
        for c in copies:
            c.wait()

    id_copies = [cp(ids_hbm, ids, id_sem.at[0]), cp(hot_hbm, hot_ids, id_sem.at[1])]
    x_copies = [cp(x_hbm.at[:, pl.ds(n * TN, TN)], xy.at[n], x_sem.at[n]) for n in range(d_tiles)]
    at_hot = [cp(hag_hbm, at.at[0, hot_cols], at_sem.at[0]), cp(hau_hbm, at.at[1, hot_cols], at_sem.at[1])]
    at_own = [cp(ag_hbm, at.at[0, own_cols], at_sem.at[2]), cp(au_hbm, at.at[1, own_cols], at_sem.at[3])]
    start(id_copies)
    start(x_copies)
    start(at_hot)
    start(gu_copies(0, 0, False))
    start(gu_copies(1, 1, False))

    barrier = pltpu.get_barrier_semaphore()
    for d in range(1, group):
        pl.semaphore_signal(barrier, inc=1, device_id={"data": lax.rem(me + d, group)}, device_id_type=MESH)

    wait(id_copies)
    pos, cls = positions(ids[...], hot_ids, n_hot, group, n_local, cap)
    place = jnp.broadcast_to(pos.astype(jnp.int32), (tokens, tokens))
    perm = (place == lax.broadcasted_iota(jnp.int32, (tokens, tokens), 0)).astype(BF16)
    cls_rows = dot_t(perm, jnp.broadcast_to(cls, (128, tokens)).astype(BF16)).astype(BF16)
    xsend[:, pl.ds(d_model, 128)] = cls_rows[half:]
    xa[kept, pl.ds(d_model, 128)] = cls_rows[:half]
    for n in range(d_tiles):
        cols = pl.ds(n * TN, TN)
        x_copies[n].wait()
        moved = dot(perm, xy[n])
        xsend[:, cols] = moved[half:].astype(BF16)
        xa[kept, cols] = moved[:half].astype(BF16)

    pl.semaphore_wait(barrier, group - 1)
    my_block = pl.ds(pl.multiple_of(me * cap, cap), cap)
    my_rows = pl.ds(pl.multiple_of(half + me * cap, cap), cap)

    def x_remote(d):
        to = lax.rem(me + d, group)
        return pltpu.make_async_remote_copy(
            src_ref=xsend.at[pl.ds(pl.multiple_of(to * cap, cap), cap)], dst_ref=xa.at[my_rows],
            send_sem=s1.at[d], recv_sem=r1.at[d], device_id={"data": to}, device_id_type=MESH)

    for d in range(1, group):
        x_remote(d).start()
    xa[my_rows, :] = xsend[my_block, :]
    pos_col = jnp.transpose(jnp.broadcast_to(pos, (128, tokens)))[:, 0:1].astype(jnp.int32)
    unperm[...] = (pos_col == lax.broadcasted_iota(jnp.int32, (tokens, tokens), 1)).astype(BF16)

    def lora(low, b):
        return (scale * dot(low, b)).astype(BF16).astype(F32)

    def act(g, u):
        return (g * jax.nn.sigmoid(g) * u).astype(BF16)

    cls_kept = xa[kept, pl.ds(d_model, 128)].astype(F32)
    for i, p in ((0, pg), (1, pu)):
        at_hot[i].wait()
        low = dot_t(xa[kept, pl.ds(0, d_model)], at[i, hot_cols, :])
        p[kept, hot_cols] = masked(low.astype(BF16).astype(F32), cls_kept, hot_group, rank)

    def first_step(s, carry):
        slot = lax.rem(s, 3)
        ahead = lax.rem(s + 2, 3)
        wait(gu_copies(s, slot, False))

        @pl.when(s + 2 < FIRST)
        def _():
            start(gu_copies(s + 2, ahead, False))

        @pl.when(s + 2 >= FIRST)
        def _():
            start(gu_copies(s + 2 - FIRST, ahead, True))

        @pl.when(s == 0)
        def _():
            start(at_own)

        xk = xa[kept, pl.ds(0, d_model)]
        g = dot(xk, wbuf[2 * slot]) + lora(pg[kept, hot_cols], bbuf[slot, 0, hot_cols, :])
        u = dot(xk, wbuf[2 * slot + 1]) + lora(pu[kept, hot_cols], bbuf[slot, 1, hot_cols, :])
        h[kept, tile_cols(s)] = act(g, u)
        return carry

    lax.fori_loop(0, FIRST, first_step, 0)

    for d in range(1, group):
        x_remote(d).wait_recv()
    cls_recv = xa[recv, pl.ds(d_model, 128)].astype(F32)
    for i, p in ((0, pg), (1, pu)):
        at_own[i].wait()
        low = dot_t(xa[recv, pl.ds(0, d_model)], at[i])
        p[recv, :] = masked(low.astype(BF16).astype(F32), cls_recv, 0, rank)
    pd[...] = jnp.zeros_like(pd)

    def add_low(slot, cols):
        pd[kept, hot_cols] += dot_t(h[kept, cols], adbuf[slot, hot_cols, :])
        pd[recv, :] += dot_t(h[recv, cols], adbuf[slot])

    def second_step(s, carry):
        slot = lax.rem(s + FIRST, 3)
        wait(gu_copies(s, slot, True))
        start(gu_copies(s + 2, lax.rem(s + FIRST + 2, 3), True))
        cols = tile_cols(s)
        xr = xa[recv, pl.ds(0, d_model)]
        g = dot(xr, wbuf[2 * slot]) + lora(pg[recv, :], bbuf[slot, 0])
        u = dot(xr, wbuf[2 * slot + 1]) + lora(pu[recv, :], bbuf[slot, 1])
        h[recv, cols] = act(g, u)
        add_low(slot, cols)
        return carry

    lax.fori_loop(0, FIRST, second_step, 0)

    def third_step(s, carry):
        slot = lax.rem(s + FIRST, 3)
        wait(gu_copies(s, slot, True))

        @pl.when(s + 2 < n_tiles)
        def _():
            start(gu_copies(s + 2, lax.rem(s + FIRST + 2, 3), True))

        @pl.when(s + 2 == n_tiles)
        def _():
            start(down_copies(0, (0, 1, 3, 4)))

        @pl.when(s + 1 == n_tiles)
        def _():
            start(down_copies(0, (2,)))
            start(down_copies(1, (0, 3, 4)))

        cols = tile_cols(s)
        xx = xa[:, pl.ds(0, d_model)]
        g = dot(xx, wbuf[2 * slot])
        u = dot(xx, wbuf[2 * slot + 1])
        gk, gr = lora(pg[kept, hot_cols], bbuf[slot, 0, hot_cols, :]), lora(pg[recv, :], bbuf[slot, 0])
        uk, ur = lora(pu[kept, hot_cols], bbuf[slot, 1, hot_cols, :]), lora(pu[recv, :], bbuf[slot, 1])
        h[kept, cols] = act(g[:half] + gk, u[:half] + uk)
        h[recv, cols] = act(g[half:] + gr, u[half:] + ur)
        add_low(slot, cols)
        return carry

    lax.fori_loop(FIRST, n_tiles, third_step, 0)
    start(down_copies(1, (1, 2)))

    pdm[kept, hot_cols] = masked(pd[kept, hot_cols].astype(BF16).astype(F32), cls_kept, hot_group, rank)
    pdm[recv, :] = masked(pd[recv, :].astype(BF16).astype(F32), cls_recv, 0, rank)

    back_rows = pl.ds(pl.multiple_of(half + me * cap, cap), cap)

    def y_remote(n, d):
        to = lax.rem(me + d, group)
        return pltpu.make_async_remote_copy(
            src_ref=xy.at[n, pl.ds(pl.multiple_of(to * cap, cap), cap)], dst_ref=xy.at[n, back_rows],
            send_sem=s2.at[n, d], recv_sem=r2.at[n, d], device_id={"data": to}, device_id_type=MESH)

    def rows_out(n, rows, low):
        y = low
        for i, (k, size) in enumerate(k_parts):
            y = dot(h[rows, pl.ds(k, size)], wbuf[down_half(n, i), pl.ds(0, size), :]) + y
        return (xa[rows, tile_cols(n)].astype(F32) + y).astype(BF16)

    def down_recv(n):
        xy[n, kept, :] = rows_out(n, recv, lora(pdm[recv, :], bbuf[down_b(n), 0]))
        for d in range(1, group):
            y_remote(n, d).start()
        xy[n, back_rows, :] = xy[n, my_block, :]

    def down_kept(n):
        y_kept[n] = rows_out(n, kept, lora(pdm[kept, hot_cols], bbuf[down_b(n), 0, hot_cols, :]))

    def out_copy(n):
        slot = lax.rem(n, 2)
        return cp(o_stage.at[slot], out_hbm.at[:, tile_cols(n)], o_sem.at[slot])

    def finish(n):
        for d in range(1, group):
            y_remote(n, d).wait_recv()
        o_stage[lax.rem(n, 2)] = (dot(unperm[:, kept], y_kept[n]) + dot(unperm[:, recv], xy[n, recv, :])).astype(BF16)
        out_copy(n).start()

    def down_step(n, carry):
        wait(down_copies(n))

        @pl.when(n > 0)
        def _():
            start(down_copies(n + 1))

        down_recv(n)
        down_kept(n)

        @pl.when(n > 0)
        def _():
            @pl.when(n > 2)
            def _():
                out_copy(n - 3).wait()
            finish(n - 1)
        return carry

    last = d_tiles - 1
    lax.fori_loop(0, last - 1, down_step, 0)
    wait(down_copies(last - 1))
    start(down_copies(last))
    down_recv(last - 1)
    out_copy(last - 4).wait()
    finish(last - 2)
    wait(down_copies(last))
    down_recv(last)
    down_kept(last - 1)
    down_kept(last)
    out_copy(last - 3).wait()
    finish(last - 1)
    out_copy(last - 2).wait()
    finish(last)
    out_copy(last - 1).wait()
    out_copy(last).wait()

    for d in range(1, group):
        x_remote(d).wait_send()

    def drain(n, carry):
        for d in range(1, group):
            y_remote(n, d).wait_send()
        return carry

    lax.fori_loop(0, d_tiles, drain, 0)


def solution(mesh):
    group = mesh.shape["data"]
    token_spec = P(("replica", "data"), None)
    store_spec = P("data", None, None)
    full_mat = P(None, None)
    full_set = P(None, None, None)
    in_specs = (token_spec, P(("replica", "data")), full_mat, full_mat, full_mat) + (store_spec,) * 6 + (P(None),) + (full_set,) * 6

    def device_step(x, adapter_id, w_gate, w_up, w_down, a_gate, b_gate, a_up, b_up, a_down, b_down, hot_ids, hot_a_gate, hot_b_gate, hot_a_up, hot_b_up, hot_a_down, hot_b_down):
        tokens, d_model = x.shape
        d_ff = w_gate.shape[1]
        n_local, _, rank = a_gate.shape
        n_hot = hot_ids.shape[0]
        cap = tokens // (2 * group)
        half = group * cap
        n_all = (n_local + n_hot) * rank
        d_tiles = d_model // TN

        def a_t(a):
            return jnp.swapaxes(a, 1, 2).reshape(a.shape[0] * rank, a.shape[1])

        def b_flat(b):
            return b.reshape(b.shape[0] * rank, b.shape[2])

        hbm = pl.BlockSpec(memory_space=pl.ANY)
        kernel = functools.partial(mlp_kernel, group, n_local, n_hot, rank, LORA_ALPHA / rank)
        return pl.pallas_call(
            kernel,
            out_shape=jax.ShapeDtypeStruct(x.shape, x.dtype),
            in_specs=[hbm] * 18,
            out_specs=hbm,
            scratch_shapes=[
                pltpu.SMEM((n_hot,), jnp.int32),
                pltpu.VMEM((1, tokens), jnp.int32),
                pltpu.VMEM((d_tiles, tokens, TN), BF16),
                pltpu.VMEM((half, d_model + 128), BF16),
                pltpu.VMEM((tokens, d_model + 128), BF16),
                pltpu.VMEM((tokens, d_ff), BF16),
                pltpu.VMEM((tokens, n_all), BF16),
                pltpu.VMEM((tokens, n_all), BF16),
                pltpu.VMEM((tokens, n_all), F32),
                pltpu.VMEM((tokens, n_all), BF16),
                pltpu.VMEM((2, n_all, d_model), BF16),
                pltpu.VMEM((6, d_model, TN), BF16),
                pltpu.VMEM((3, 2, n_all, TN), BF16),
                pltpu.VMEM((3, n_all, TN), BF16),
                pltpu.VMEM((d_tiles, half, TN), BF16),
                pltpu.VMEM((2, tokens, TN), BF16),
                pltpu.VMEM((tokens, tokens), BF16),
                pltpu.SemaphoreType.DMA((2,)),
                pltpu.SemaphoreType.DMA((d_tiles,)),
                pltpu.SemaphoreType.DMA((4,)),
                pltpu.SemaphoreType.DMA((3, 8)),
                pltpu.SemaphoreType.DMA((2, 5)),
                pltpu.SemaphoreType.DMA((2,)),
                pltpu.SemaphoreType.DMA((group,)),
                pltpu.SemaphoreType.DMA((group,)),
                pltpu.SemaphoreType.DMA((d_tiles, group)),
                pltpu.SemaphoreType.DMA((d_tiles, group)),
            ],
            compiler_params=pltpu.CompilerParams(
                collective_id=0, has_side_effects=True, vmem_limit_bytes=67043328),
        )(hot_ids, adapter_id.reshape(1, tokens), x, w_gate, w_up, w_down,
          a_t(a_gate), b_flat(b_gate), a_t(a_up), b_flat(b_up), a_t(a_down), b_flat(b_down),
          a_t(hot_a_gate), b_flat(hot_b_gate), a_t(hot_a_up), b_flat(hot_b_up), a_t(hot_a_down), b_flat(hot_b_down))

    return jax.shard_map(device_step, mesh=mesh, in_specs=in_specs, out_specs=token_spec, check_vma=False)
```

```python
import functools

import jax
import jax.numpy as jnp
from jax import lax
from jax.experimental import pallas as pl
from jax.experimental.pallas import tpu as pltpu
from jax.sharding import PartitionSpec as P

LORA_ALPHA = 32
MESH = pl.DeviceIdType.MESH
F32 = jnp.float32
BF16 = jnp.bfloat16

TN = 512
FIRST = 10


def dot(a, b):
    return jnp.dot(a, b, preferred_element_type=F32)


def dot_t(a, b):
    return lax.dot_general(a, b, (((1,), (1,)), ((), ())), preferred_element_type=F32)


def positions(ids, hot_ids, n_hot, group, n_local, cap):
    tokens = ids.shape[1]
    kept = tokens - group * cap
    is_hot = ids < 0
    hot_idx = jnp.zeros_like(ids)
    for j in range(n_hot):
        match = ids == hot_ids[j]
        is_hot = is_hot | match
        hot_idx = jnp.where(match, j, hot_idx)
    owner = jnp.where(is_hot, group, ids // n_local)
    local = ids - (ids // n_local) * n_local
    cls = jnp.where(is_hot, n_local + hot_idx, local)
    rows = 2 * group
    kind = lax.broadcasted_iota(jnp.int32, (rows, tokens), 0)
    member = (kind == jnp.broadcast_to(owner, (rows, tokens))).astype(F32)
    before = lax.broadcasted_iota(jnp.int32, (tokens, tokens), 0) < lax.broadcasted_iota(jnp.int32, (tokens, tokens), 1)
    cum = dot(member.astype(BF16), before.astype(BF16))
    rank = jnp.sum(member * cum, axis=0, keepdims=True)
    counts = jnp.sum(member, axis=1, keepdims=True)
    sub = lax.broadcasted_iota(jnp.int32, (rows, 1), 0)
    holes = jnp.where(sub < group, cap - counts, 0.0)
    lower = lax.broadcasted_iota(jnp.int32, (rows, rows), 1) < lax.broadcasted_iota(jnp.int32, (rows, rows), 0)
    hole_start = dot(lower.astype(BF16), jnp.broadcast_to(holes, (rows, 128)).astype(BF16))[:, 0:1]
    spill = jnp.broadcast_to(rank - kept, (rows, tokens))
    takes = (spill >= hole_start) & (spill < hole_start + holes)
    base = kept + cap * sub.astype(F32) + counts - hole_start
    filled = jnp.sum(jnp.where(takes, base + spill, 0.0), axis=0, keepdims=True)
    own = kept + cap * owner.astype(F32) + rank
    pos = jnp.where(is_hot, jnp.where(rank < kept, rank, filled), own)
    return pos, cls.astype(F32)


def masked(low, cls, first_group, rank):
    per = 128 // rank
    lane = lax.broadcasted_iota(jnp.int32, (low.shape[0], 128), 1) // rank
    parts = []
    for k in range(low.shape[1] // 128):
        here = (lane + per * (first_group + k)).astype(F32) == cls
        parts.append(jnp.where(here, low[:, k * 128:(k + 1) * 128], 0.0).astype(BF16))
    return jnp.concatenate(parts, axis=1)


def mlp_kernel(group, n_local, n_hot, rank, scale,
               hot_hbm, ids_hbm, x_hbm, wg_hbm, wu_hbm, wd_hbm,
               ag_hbm, bg_hbm, au_hbm, bu_hbm, ad_hbm, bd_hbm,
               hag_hbm, hbg_hbm, hau_hbm, hbu_hbm, had_hbm, hbd_hbm,
               y_hbm, unperm_hbm,
               hot_ids, ids, xy, xsend, xa, h, pg, pu, pd, pdm, wbuf, bbuf, adbuf, unperm,
               id_sem, x_sem, at_sem, w_sem, ad_sem, d_sem, y_sem, p_sem, s1, r1, s2, r2):
    me = lax.axis_index("data")
    tokens, d_model = x_hbm.shape
    d_ff = wg_hbm.shape[1]
    cap = tokens // (2 * group)
    half = group * cap
    n_own = n_local * rank
    n_hr = n_hot * rank
    n_all = n_own + n_hr
    n_tiles = d_ff // TN
    d_tiles = d_model // TN
    kept = pl.ds(0, half)
    recv = pl.ds(half, half)
    own_cols = pl.ds(0, n_own)
    hot_cols = pl.ds(n_own, n_hr)
    hot_group = n_own // 128
    lead = (FIRST - 1 + n_tiles) % 3
    k_parts = [(k, min(d_model, d_ff - k)) for k in range(0, d_ff, d_model)]
    assert len(k_parts) == 3

    def cp(src, dst, sem):
        return pltpu.make_async_copy(src, dst, sem)

    def tile_cols(tile):
        return pl.ds(tile * TN if isinstance(tile, int) else pl.multiple_of(tile * TN, TN), TN)

    def gu_base(tile, slot):
        cols = tile_cols(tile)
        return [
            cp(wg_hbm.at[:, cols], wbuf.at[2 * slot], w_sem.at[slot, 0]),
            cp(wu_hbm.at[:, cols], wbuf.at[2 * slot + 1], w_sem.at[slot, 1]),
            cp(hbg_hbm.at[:, cols], bbuf.at[slot, 0, hot_cols], w_sem.at[slot, 2]),
            cp(hbu_hbm.at[:, cols], bbuf.at[slot, 1, hot_cols], w_sem.at[slot, 3]),
        ]

    def gu_extra(tile, slot, ad_slot):
        cols = tile_cols(tile)
        return [
            cp(bg_hbm.at[:, cols], bbuf.at[slot, 0, own_cols], w_sem.at[slot, 4]),
            cp(bu_hbm.at[:, cols], bbuf.at[slot, 1, own_cols], w_sem.at[slot, 5]),
            cp(ad_hbm.at[:, cols], adbuf.at[ad_slot, own_cols], ad_sem.at[ad_slot, 0]),
            cp(had_hbm.at[:, cols], adbuf.at[ad_slot, hot_cols], ad_sem.at[ad_slot, 1]),
        ]

    def ring(s):
        return lax.rem(s + FIRST - 1, 3)

    def gu_full(tile, s):
        return gu_base(tile, ring(s)) + gu_extra(tile, ring(s), lax.rem(s, 4))

    def a_view(i, c, first, size):
        index = i * d_tiles + c
        per = d_model // n_all
        return wbuf.at[6 + index // per, pl.ds((index % per) * n_all + first, size)]

    def a_copies(i, src, first, size, side):
        return [cp(src.at[:, pl.ds(c * TN, TN)], a_view(i, c, first, size), at_sem.at[2 * side + i, c]) for c in range(d_tiles)]

    def down_half(n, i):
        k = lax.rem(n, 3)
        return jnp.where(k == 0, 6 + i, lax.rem(2 * lead + 3 * (k + 1) + i, 6))

    def down_b(n):
        k = lax.rem(n, 3)
        return lax.rem(lead + k // 2, 3), lax.rem(k, 2)

    def down_copies(n, pieces=(0, 1, 2, 3, 4)):
        cols = tile_cols(n)
        out = []
        for i in pieces:
            if i < 3:
                k, size = k_parts[i]
                src, dst = wd_hbm.at[pl.ds(k, size), cols], wbuf.at[down_half(n, i), pl.ds(0, size)]
            elif i == 3:
                src, dst = bd_hbm.at[:, cols], bbuf.at[down_b(n)[0], down_b(n)[1], own_cols]
            else:
                src, dst = hbd_hbm.at[:, cols], bbuf.at[down_b(n)[0], down_b(n)[1], hot_cols]
            out.append(cp(src, dst, d_sem.at[lax.rem(n, 3), i]))
        return out

    def start(copies):
        for c in copies:
            c.start()

    def wait(copies):
        for c in copies:
            c.wait()

    id_copies = [cp(ids_hbm, ids, id_sem.at[0]), cp(hot_hbm, hot_ids, id_sem.at[1])]
    x_copies = [cp(x_hbm.at[:, pl.ds(n * TN, TN)], xy.at[n], x_sem.at[n]) for n in range(d_tiles)]
    a_hot = a_copies(0, hag_hbm, n_own, n_hr, 0) + a_copies(1, hau_hbm, n_own, n_hr, 0)
    a_own = a_copies(0, ag_hbm, 0, n_own, 1) + a_copies(1, au_hbm, 0, n_own, 1)
    start(id_copies)
    start(x_copies)
    start(a_hot)
    start(gu_base(0, 0))
    start(gu_base(1, 1))

    barrier = pltpu.get_barrier_semaphore()
    for d in range(1, group):
        pl.semaphore_signal(barrier, inc=1, device_id={"data": lax.rem(me + d, group)}, device_id_type=MESH)

    wait(id_copies)
    pos, cls = positions(ids[...], hot_ids, n_hot, group, n_local, cap)
    place = jnp.broadcast_to(pos.astype(jnp.int32), (tokens, tokens))
    perm = (place == lax.broadcasted_iota(jnp.int32, (tokens, tokens), 0)).astype(BF16)
    cls_rows = dot_t(perm, jnp.broadcast_to(cls, (128, tokens)).astype(BF16)).astype(BF16)
    xsend[:, pl.ds(d_model, 128)] = cls_rows[half:]
    xa[kept, pl.ds(d_model, 128)] = cls_rows[:half]
    wait(x_copies)
    for n in range(d_tiles):
        cols = pl.ds(n * TN, TN)
        moved = dot(perm, xy[n])
        xsend[:, cols] = moved[half:].astype(BF16)
        xa[kept, cols] = moved[:half].astype(BF16)

    pl.semaphore_wait(barrier, group - 1)
    my_block = pl.ds(pl.multiple_of(me * cap, cap), cap)
    my_rows = pl.ds(pl.multiple_of(half + me * cap, cap), cap)

    def x_remote(d):
        to = lax.rem(me + d, group)
        return pltpu.make_async_remote_copy(
            src_ref=xsend.at[pl.ds(pl.multiple_of(to * cap, cap), cap)], dst_ref=xa.at[my_rows],
            send_sem=s1.at[d], recv_sem=r1.at[d], device_id={"data": to}, device_id_type=MESH)

    for d in range(1, group):
        x_remote(d).start()
    wait(a_hot)
    xa[my_rows, :] = xsend[my_block, :]
    pos_col = jnp.transpose(jnp.broadcast_to(pos, (128, tokens)))[:, 0:1].astype(jnp.int32)
    unperm[...] = (pos_col == lax.broadcasted_iota(jnp.int32, (tokens, tokens), 1)).astype(BF16)

    def delta(low, b):
        return (scale * dot(low, b)).astype(BF16)

    def act(g, u, dg, du):
        g = g + dg.astype(F32)
        u = u + du.astype(F32)
        return (g * jax.nn.sigmoid(g) * u).astype(BF16)

    def low_rank(rows, first, size):
        low = [None, None]
        for c in range(d_tiles):
            for i in range(2):
                part = dot_t(xa[rows, pl.ds(c * TN, TN)], a_view(i, c, first, size)[...])
                low[i] = part if low[i] is None else low[i] + part
        return low

    def masked_bf16(low, cls, first_group):
        return masked(low.astype(BF16).astype(F32), cls, first_group, rank)

    cls_kept = xa[kept, pl.ds(d_model, 128)].astype(F32)
    low_g, low_u = low_rank(kept, n_own, n_hr)
    pg[kept, hot_cols] = masked_bf16(low_g, cls_kept, hot_group)
    pu[kept, hot_cols] = masked_bf16(low_u, cls_kept, hot_group)

    def first_step(s, carry):
        slot = lax.rem(s, 3)
        ahead = lax.rem(s + 2, 3)
        wait(gu_base(s, slot))

        @pl.when(s + 2 < FIRST)
        def _():
            start(gu_base(s + 2, ahead))

        @pl.when(s + 3 == FIRST)
        def _():
            start(gu_extra(FIRST - 1, ahead, 0))

        @pl.when(s + 2 >= FIRST)
        def _():
            start(gu_full(s + 2 - FIRST, s + 3 - FIRST))

        @pl.when(s == 1)
        def _():
            start(a_own)

        xk = xa[kept, pl.ds(0, d_model)]
        dg = delta(pg[kept, hot_cols], bbuf[slot, 0, hot_cols, :])
        du = delta(pu[kept, hot_cols], bbuf[slot, 1, hot_cols, :])
        h[kept, tile_cols(s)] = act(dot(xk, wbuf[2 * slot]), dot(xk, wbuf[2 * slot + 1]), dg, du)
        return carry

    lax.fori_loop(0, FIRST, first_step, 0)

    cp(unperm, unperm_hbm, p_sem).start()
    wait(a_own)
    for d in range(1, group):
        x_remote(d).wait_recv()
    cls_recv = xa[recv, pl.ds(d_model, 128)].astype(F32)
    low_g, low_u = low_rank(recv, 0, n_all)
    pg[recv, :] = masked_bf16(low_g, cls_recv, 0)
    pu[recv, :] = masked_bf16(low_u, cls_recv, 0)
    pd[...] = jnp.zeros_like(pd)

    def add_low(tile, ad_slot):
        cols = tile_cols(tile)
        low_kept = dot_t(h[kept, cols], adbuf[ad_slot, hot_cols, :])
        low_recv = dot_t(h[recv, cols], adbuf[ad_slot])
        pd[kept, hot_cols] += low_kept
        pd[recv, :] += low_recv

    def recv_tile(tile, slot, between):
        xr = xa[recv, pl.ds(0, d_model)]
        dg, du = delta(pg[recv, :], bbuf[slot, 0]), delta(pu[recv, :], bbuf[slot, 1])
        g, u = dot(xr, wbuf[2 * slot]), dot(xr, wbuf[2 * slot + 1])
        between()
        h[recv, tile_cols(tile)] = act(g, u, dg, du)

    wait(gu_extra(FIRST - 1, (FIRST - 1) % 3, 0))
    recv_tile(FIRST - 1, (FIRST - 1) % 3, lambda: None)

    def second_step(s, carry):
        wait(gu_full(s - 1, s))
        start(gu_full(jnp.where(s + 2 < FIRST, s + 1, s + 2), s + 2))
        recv_tile(s - 1, ring(s), lambda: add_low(jnp.where(s == 1, FIRST - 1, s - 2), lax.rem(s + 3, 4)))
        return carry

    lax.fori_loop(1, FIRST, second_step, 0)

    def third_step(s, carry):
        slot = ring(s)
        wait(gu_full(s, s))

        @pl.when(s + 2 < n_tiles)
        def _():
            start(gu_full(s + 2, s + 2))

        @pl.when(s == FIRST)
        def _():
            start(down_copies(0, (0, 1, 2)))

        @pl.when(s + 2 == n_tiles)
        def _():
            start(down_copies(0, (3, 4)) + down_copies(1, (0, 1, 3, 4)))

        @pl.when(s + 1 == n_tiles)
        def _():
            start(down_copies(1, (2,)) + down_copies(2, (0, 3, 4)))

        xx = xa[:, pl.ds(0, d_model)]
        dgk = delta(pg[kept, hot_cols], bbuf[slot, 0, hot_cols, :])
        dgr = delta(pg[recv, :], bbuf[slot, 0])
        duk = delta(pu[kept, hot_cols], bbuf[slot, 1, hot_cols, :])
        dur = delta(pu[recv, :], bbuf[slot, 1])
        g, u = dot(xx, wbuf[2 * slot]), dot(xx, wbuf[2 * slot + 1])
        add_low(jnp.where(s == FIRST, FIRST - 2, s - 1), lax.rem(s + 3, 4))
        h[kept, tile_cols(s)] = act(g[:half], u[:half], dgk, duk)
        h[recv, tile_cols(s)] = act(g[half:], u[half:], dgr, dur)
        return carry

    lax.fori_loop(FIRST, n_tiles, third_step, 0)
    start(down_copies(2, (1, 2)))
    add_low(n_tiles - 1, (n_tiles - 1) % 4)

    pdm[kept, hot_cols] = masked_bf16(pd[kept, hot_cols], cls_kept, hot_group)
    pdm[recv, :] = masked_bf16(pd[recv, :], cls_recv, 0)

    def y_remote(n, d):
        to = lax.rem(me + d, group)
        return pltpu.make_async_remote_copy(
            src_ref=xy.at[n, pl.ds(pl.multiple_of(to * cap, cap), cap)], dst_ref=y_hbm.at[my_rows, tile_cols(n)],
            send_sem=s2.at[n, d], recv_sem=r2.at[n, d], device_id={"data": to}, device_id_type=MESH)

    def y_local(n):
        return [cp(xy.at[n, recv], y_hbm.at[kept, tile_cols(n)], y_sem.at[n, 0])]

    def y_self(n):
        return [cp(xy.at[n, my_block], y_hbm.at[my_rows, tile_cols(n)], y_sem.at[n, 1])]

    def rows_out(n, rows, low):
        y = low
        for i, (k, size) in enumerate(k_parts):
            y = dot(h[rows, pl.ds(k, size)], wbuf[down_half(n, i), pl.ds(0, size), :]) + y
        return (xa[rows, tile_cols(n)].astype(F32) + y).astype(BF16)

    def down_recv(n):
        slot, part = down_b(n)
        xy[n, kept, :] = rows_out(n, recv, delta(pdm[recv, :], bbuf[slot, part]).astype(F32))

    def down_kept(n):
        slot, part = down_b(n)
        xy[n, recv, :] = rows_out(n, kept, delta(pdm[kept, hot_cols], bbuf[slot, part, hot_cols, :]).astype(F32))

    def send_back(n):
        for d in range(1, group):
            y_remote(n, d).start()
        start(y_self(n))

    def down_step(n, carry):
        wait(down_copies(n))

        @pl.when(n > 0)
        def _():
            start(down_copies(n + 2))

        down_recv(n)
        down_kept(n)
        send_back(n)
        start(y_local(n))
        return carry

    last = d_tiles - 1
    lax.fori_loop(0, last - 1, down_step, 0)
    wait(down_copies(last - 1))
    wait(down_copies(last))
    down_recv(last - 1)
    send_back(last - 1)
    down_recv(last)
    send_back(last)
    down_kept(last - 1)
    down_kept(last)
    start(y_local(last - 1) + y_local(last))

    for d in range(1, group):
        x_remote(d).wait_send()
    cp(unperm, unperm_hbm, p_sem).wait()

    def drain(n, carry):
        wait(y_self(n) + y_local(n))
        for d in range(1, group):
            y_remote(n, d).wait_send()
            y_remote(n, d).wait_recv()
        return carry

    lax.fori_loop(0, d_tiles, drain, 0)


def place_kernel(y_hbm, unperm_hbm, out_hbm, y, unperm, out, y_sem, p_sem, o_sem):
    tiles = y.shape[0]

    def y_copy(n):
        return pltpu.make_async_copy(y_hbm.at[:, pl.ds(n * TN, TN)], y.at[n], y_sem.at[n])

    def o_copy(n):
        return pltpu.make_async_copy(out.at[n], out_hbm.at[:, pl.ds(n * TN, TN)], o_sem.at[n])

    p_copy = pltpu.make_async_copy(unperm_hbm, unperm, p_sem)
    p_copy.start()
    for n in range(tiles):
        y_copy(n).start()
    p_copy.wait()
    for n in range(tiles):
        y_copy(n).wait()
        out[n] = dot(unperm[...], y[n]).astype(BF16)
        o_copy(n).start()
    for n in range(tiles):
        o_copy(n).wait()


def solution(mesh):
    group = mesh.shape["data"]
    token_spec = P(("replica", "data"), None)
    store_spec = P("data", None, None)
    full_mat = P(None, None)
    full_set = P(None, None, None)
    in_specs = (token_spec, P(("replica", "data")), full_mat, full_mat, full_mat) + (store_spec,) * 6 + (P(None),) + (full_set,) * 6

    def device_step(x, adapter_id, w_gate, w_up, w_down, a_gate, b_gate, a_up, b_up, a_down, b_down, hot_ids, hot_a_gate, hot_b_gate, hot_a_up, hot_b_up, hot_a_down, hot_b_down):
        tokens, d_model = x.shape
        d_ff = w_gate.shape[1]
        n_local, _, rank = a_gate.shape
        n_hot = hot_ids.shape[0]
        cap = tokens // (2 * group)
        half = group * cap
        n_all = (n_local + n_hot) * rank
        d_tiles = d_model // TN

        def a_t(a):
            return jnp.swapaxes(a, 1, 2).reshape(a.shape[0] * rank, a.shape[1])

        def b_flat(b):
            return b.reshape(b.shape[0] * rank, b.shape[2])

        hbm = pl.BlockSpec(memory_space=pl.ANY)
        kernel = functools.partial(mlp_kernel, group, n_local, n_hot, rank, LORA_ALPHA / rank)
        y, unperm = pl.pallas_call(
            kernel,
            out_shape=(jax.ShapeDtypeStruct(x.shape, x.dtype), jax.ShapeDtypeStruct((tokens, tokens), BF16)),
            in_specs=[hbm] * 18,
            out_specs=(hbm, hbm),
            scratch_shapes=[
                pltpu.SMEM((n_hot,), jnp.int32),
                pltpu.VMEM((1, tokens), jnp.int32),
                pltpu.VMEM((d_tiles, tokens, TN), BF16),
                pltpu.VMEM((half, d_model + 128), BF16),
                pltpu.VMEM((tokens, d_model + 128), BF16),
                pltpu.VMEM((tokens, d_ff), BF16),
                pltpu.VMEM((tokens, n_all), BF16),
                pltpu.VMEM((tokens, n_all), BF16),
                pltpu.VMEM((tokens, n_all), F32),
                pltpu.VMEM((tokens, n_all), BF16),
                pltpu.VMEM((9, d_model, TN), BF16),
                pltpu.VMEM((3, 2, n_all, TN), BF16),
                pltpu.VMEM((4, n_all, TN), BF16),
                pltpu.VMEM((tokens, tokens), BF16),
                pltpu.SemaphoreType.DMA((2,)),
                pltpu.SemaphoreType.DMA((d_tiles,)),
                pltpu.SemaphoreType.DMA((4, d_tiles)),
                pltpu.SemaphoreType.DMA((3, 6)),
                pltpu.SemaphoreType.DMA((4, 2)),
                pltpu.SemaphoreType.DMA((3, 5)),
                pltpu.SemaphoreType.DMA((d_tiles, 2)),
                pltpu.SemaphoreType.DMA,
                pltpu.SemaphoreType.DMA((group,)),
                pltpu.SemaphoreType.DMA((group,)),
                pltpu.SemaphoreType.DMA((d_tiles, group)),
                pltpu.SemaphoreType.DMA((d_tiles, group)),
            ],
            compiler_params=pltpu.CompilerParams(
                collective_id=0, has_side_effects=True, vmem_limit_bytes=67043328),
        )(hot_ids, adapter_id.reshape(1, tokens), x, w_gate, w_up, w_down,
          a_t(a_gate), b_flat(b_gate), a_t(a_up), b_flat(b_up), a_t(a_down), b_flat(b_down),
          a_t(hot_a_gate), b_flat(hot_b_gate), a_t(hot_a_up), b_flat(hot_b_up), a_t(hot_a_down), b_flat(hot_b_down))
        return pl.pallas_call(
            place_kernel,
            out_shape=jax.ShapeDtypeStruct(x.shape, x.dtype),
            in_specs=[hbm] * 2,
            out_specs=hbm,
            scratch_shapes=[
                pltpu.VMEM((d_tiles, tokens, TN), BF16),
                pltpu.VMEM((tokens, tokens), BF16),
                pltpu.VMEM((d_tiles, tokens, TN), BF16),
                pltpu.SemaphoreType.DMA((d_tiles,)),
                pltpu.SemaphoreType.DMA,
                pltpu.SemaphoreType.DMA((d_tiles,)),
            ],
        )(y, unperm)

    return jax.shard_map(device_step, mesh=mesh, in_specs=in_specs, out_specs=token_spec, check_vma=False)
```

```python
import functools

import jax
import jax.numpy as jnp
from jax import lax
from jax.experimental import pallas as pl
from jax.experimental.pallas import tpu as pltpu
from jax.sharding import PartitionSpec as P

LORA_ALPHA = 32
MESH = pl.DeviceIdType.MESH
F32 = jnp.float32
BF16 = jnp.bfloat16

TN = 512
FIRST = 8


def dot(a, b):
    return jnp.dot(a, b, preferred_element_type=F32)


def dot_t(a, b):
    return lax.dot_general(a, b, (((1,), (1,)), ((), ())), preferred_element_type=F32)


def earlier(tokens):
    row = lax.broadcasted_iota(jnp.int32, (tokens, tokens), 0)
    return (row < lax.broadcasted_iota(jnp.int32, (tokens, tokens), 1)).astype(BF16)


def positions(ids, hot_ids, before, n_hot, group, n_local, cap):
    tokens = ids.shape[1]
    kept = tokens - group * cap
    is_hot = ids < 0
    hot_idx = jnp.zeros_like(ids)
    for j in range(n_hot):
        match = ids == hot_ids[j]
        is_hot = is_hot | match
        hot_idx = jnp.where(match, j, hot_idx)
    owner = jnp.where(is_hot, group, ids // n_local)
    local = ids - (ids // n_local) * n_local
    cls = jnp.where(is_hot, n_local + hot_idx, local)
    rows = 2 * group
    kind = lax.broadcasted_iota(jnp.int32, (rows, tokens), 0)
    member = (kind == jnp.broadcast_to(owner, (rows, tokens))).astype(F32)
    cum = dot(member.astype(BF16), before)
    rank = jnp.sum(member * cum, axis=0, keepdims=True)
    counts = jnp.sum(member, axis=1, keepdims=True)
    sub = lax.broadcasted_iota(jnp.int32, (rows, 1), 0)
    holes = jnp.where(sub < group, cap - counts, 0.0)
    lower = lax.broadcasted_iota(jnp.int32, (rows, rows), 1) < lax.broadcasted_iota(jnp.int32, (rows, rows), 0)
    hole_start = dot(lower.astype(BF16), jnp.broadcast_to(holes, (rows, 128)).astype(BF16))[:, 0:1]
    spill = jnp.broadcast_to(rank - kept, (rows, tokens))
    takes = (spill >= hole_start) & (spill < hole_start + holes)
    base = kept + cap * sub.astype(F32) + counts - hole_start
    filled = jnp.sum(jnp.where(takes, base + spill, 0.0), axis=0, keepdims=True)
    own = kept + cap * owner.astype(F32) + rank
    pos = jnp.where(is_hot, jnp.where(rank < kept, rank, filled), own)
    return pos, cls.astype(F32)


def masked(low, cls, first_group, rank):
    per = 128 // rank
    lane = lax.broadcasted_iota(jnp.int32, (low.shape[0], 128), 1) // rank
    parts = []
    for k in range(low.shape[1] // 128):
        here = (lane + per * (first_group + k)).astype(F32) == cls
        parts.append(jnp.where(here, low[:, k * 128:(k + 1) * 128], 0.0).astype(BF16))
    return jnp.concatenate(parts, axis=1)


def mlp_kernel(group, n_local, n_hot, rank, scale,
               hot_hbm, ids_hbm, x_hbm, wg_hbm, wu_hbm, wd_hbm,
               ag_hbm, bg_hbm, au_hbm, bu_hbm, ad_hbm, bd_hbm,
               hag_hbm, hbg_hbm, hau_hbm, hbu_hbm, had_hbm, hbd_hbm,
               y_hbm, unperm_hbm,
               hot_ids, ids, xy, xsend, xa, h, pg, pu, pd, pdm, wbuf, bbuf, adbuf, unperm,
               id_sem, x_sem, at_sem, w_sem, ad_sem, d_sem, y_sem, p_sem, s1, r1, s2, r2):
    me = lax.axis_index("data")
    tokens, d_model = x_hbm.shape
    d_ff = wg_hbm.shape[1]
    cap = tokens // (2 * group)
    half = group * cap
    n_own = n_local * rank
    n_hr = n_hot * rank
    n_all = n_own + n_hr
    n_tiles = d_ff // TN
    d_tiles = d_model // TN
    kept = pl.ds(0, half)
    recv = pl.ds(half, half)
    own_cols = pl.ds(0, n_own)
    hot_cols = pl.ds(n_own, n_hr)
    hot_group = n_own // 128
    lead = (FIRST - 1 + n_tiles) % 3
    k_parts = [(k, min(d_model, d_ff - k)) for k in range(0, d_ff, d_model)]
    assert len(k_parts) == 3 and n_tiles == 2 * FIRST

    def cp(src, dst, sem):
        return pltpu.make_async_copy(src, dst, sem)

    def tile_cols(tile):
        return pl.ds(tile * TN if isinstance(tile, int) else pl.multiple_of(tile * TN, TN), TN)

    def gu_base(tile, slot):
        cols = tile_cols(tile)
        return [
            cp(wg_hbm.at[:, cols], wbuf.at[2 * slot], w_sem.at[slot, 0]),
            cp(wu_hbm.at[:, cols], wbuf.at[2 * slot + 1], w_sem.at[slot, 1]),
            cp(hbg_hbm.at[:, cols], bbuf.at[slot, 0, hot_cols], w_sem.at[slot, 2]),
            cp(hbu_hbm.at[:, cols], bbuf.at[slot, 1, hot_cols], w_sem.at[slot, 3]),
        ]

    def gu_extra(tile, slot, ad_slot):
        cols = tile_cols(tile)
        return [
            cp(bg_hbm.at[:, cols], bbuf.at[slot, 0, own_cols], w_sem.at[slot, 4]),
            cp(bu_hbm.at[:, cols], bbuf.at[slot, 1, own_cols], w_sem.at[slot, 5]),
            cp(ad_hbm.at[:, cols], adbuf.at[ad_slot, own_cols], ad_sem.at[ad_slot, 0]),
            cp(had_hbm.at[:, cols], adbuf.at[ad_slot, hot_cols], ad_sem.at[ad_slot, 1]),
        ]

    def ring(s):
        return lax.rem(s + FIRST - 1, 3)

    def gu_full(tile, s):
        return gu_base(tile, ring(s)) + gu_extra(tile, ring(s), lax.rem(s, 4))

    def a_view(i, c, first, size):
        index = i * d_tiles + c
        per = d_model // n_all
        return wbuf.at[6 + index // per, pl.ds((index % per) * n_all + first, size)]

    def a_copies(i, src, first, size, side):
        return [cp(src.at[:, pl.ds(c * TN, TN)], a_view(i, c, first, size), at_sem.at[2 * side + i, c]) for c in range(d_tiles)]

    def down_half(n, i):
        k = lax.rem(n, 3)
        return jnp.where(k == 0, 6 + i, lax.rem(2 * lead + 3 * (k + 1) + i, 6))

    def down_b(n):
        k = lax.rem(n, 3)
        return lax.rem(lead + k // 2, 3), lax.rem(k, 2)

    def down_copies(n, pieces=(0, 1, 2, 3, 4)):
        cols = tile_cols(n)
        out = []
        for i in pieces:
            if i < 3:
                k, size = k_parts[i]
                src, dst = wd_hbm.at[pl.ds(k, size), cols], wbuf.at[down_half(n, i), pl.ds(0, size)]
            elif i == 3:
                src, dst = bd_hbm.at[:, cols], bbuf.at[down_b(n)[0], down_b(n)[1], own_cols]
            else:
                src, dst = hbd_hbm.at[:, cols], bbuf.at[down_b(n)[0], down_b(n)[1], hot_cols]
            out.append(cp(src, dst, d_sem.at[lax.rem(n, 3), i]))
        return out

    def start(copies):
        for c in copies:
            c.start()

    def wait(copies):
        for c in copies:
            c.wait()

    id_copies = [cp(ids_hbm, ids, id_sem.at[0]), cp(hot_hbm, hot_ids, id_sem.at[1])]
    x_copies = [cp(x_hbm.at[:, pl.ds(n * TN, TN)], xy.at[n], x_sem.at[n]) for n in range(d_tiles)]
    a_hot = a_copies(0, hag_hbm, n_own, n_hr, 0) + a_copies(1, hau_hbm, n_own, n_hr, 0)
    a_own = a_copies(0, ag_hbm, 0, n_own, 1) + a_copies(1, au_hbm, 0, n_own, 1)
    start(id_copies)
    start(x_copies)
    start(a_hot)
    start(gu_base(0, 0))
    start(gu_base(1, 1))

    barrier = pltpu.get_barrier_semaphore()
    for d in range(1, group):
        pl.semaphore_signal(barrier, inc=1, device_id={"data": lax.rem(me + d, group)}, device_id_type=MESH)

    before = earlier(tokens)
    wait(id_copies)
    pos, cls = positions(ids[...], hot_ids, before, n_hot, group, n_local, cap)
    place = jnp.broadcast_to(pos.astype(jnp.int32), (tokens, tokens))
    perm = (place == lax.broadcasted_iota(jnp.int32, (tokens, tokens), 0)).astype(BF16)
    cls_rows = dot_t(perm, jnp.broadcast_to(cls, (128, tokens)).astype(BF16)).astype(BF16)
    xsend[:, pl.ds(d_model, 128)] = cls_rows[half:]
    xa[kept, pl.ds(d_model, 128)] = cls_rows[:half]
    wait(x_copies)
    for n in range(d_tiles):
        xsend[:, pl.ds(n * TN, TN)] = dot(perm[half:], xy[n]).astype(BF16)

    pl.semaphore_wait(barrier, group - 1)
    my_block = pl.ds(pl.multiple_of(me * cap, cap), cap)
    my_rows = pl.ds(pl.multiple_of(half + me * cap, cap), cap)

    def x_remote(d):
        to = lax.rem(me + d, group)
        return pltpu.make_async_remote_copy(
            src_ref=xsend.at[pl.ds(pl.multiple_of(to * cap, cap), cap)], dst_ref=xa.at[my_rows],
            send_sem=s1, recv_sem=r1, device_id={"data": to}, device_id_type=MESH)

    others = (group - 1) * cap
    x_all = pltpu.make_async_remote_copy(
        src_ref=xsend.at[pl.ds(0, others)], dst_ref=xa.at[pl.ds(half, others)],
        send_sem=s1, recv_sem=r1, device_id={"data": lax.rem(me + 1, group)}, device_id_type=MESH)

    for d in range(1, group):
        x_remote(d).start()
    for n in range(d_tiles):
        xa[kept, pl.ds(n * TN, TN)] = dot(perm[:half], xy[n]).astype(BF16)
    wait(a_hot)
    xa[my_rows, :] = xsend[my_block, :]
    pos_col = jnp.transpose(jnp.broadcast_to(pos, (128, tokens)))[:, 0:1].astype(jnp.int32)
    unperm[...] = (pos_col == lax.broadcasted_iota(jnp.int32, (tokens, tokens), 1)).astype(BF16)

    def delta(low, b):
        return (scale * dot(low, b)).astype(BF16)

    def act(g, u, dg, du):
        g = g + dg.astype(F32)
        u = u + du.astype(F32)
        return (g * jax.nn.sigmoid(g) * u).astype(BF16)

    def low_rank(rows, first, size):
        low = [None, None]
        for c in range(d_tiles):
            for i in range(2):
                part = dot_t(xa[rows, pl.ds(c * TN, TN)], a_view(i, c, first, size)[...])
                low[i] = part if low[i] is None else low[i] + part
        return low

    def masked_bf16(low, cls, first_group):
        return masked(low.astype(BF16).astype(F32), cls, first_group, rank)

    cls_kept = xa[kept, pl.ds(d_model, 128)].astype(F32)
    low_g, low_u = low_rank(kept, n_own, n_hr)
    pg[kept, hot_cols] = masked_bf16(low_g, cls_kept, hot_group)
    pu[kept, hot_cols] = masked_bf16(low_u, cls_kept, hot_group)

    def first_step(s, carry):
        slot = lax.rem(s, 3)
        ahead = lax.rem(s + 2, 3)
        wait(gu_base(s, slot))

        @pl.when(s + 2 < FIRST)
        def _():
            start(gu_base(s + 2, ahead))

        @pl.when(s + 3 == FIRST)
        def _():
            start(gu_extra(FIRST - 1, ahead, 0))

        @pl.when(s + 2 >= FIRST)
        def _():
            start(gu_full(jnp.where(s + 2 == FIRST, FIRST, 0), s + 3 - FIRST))

        @pl.when(s == 1)
        def _():
            start(a_own)

        xk = xa[kept, pl.ds(0, d_model)]
        dg = delta(pg[kept, hot_cols], bbuf[slot, 0, hot_cols, :])
        du = delta(pu[kept, hot_cols], bbuf[slot, 1, hot_cols, :])
        h[kept, tile_cols(s)] = act(dot(xk, wbuf[2 * slot]), dot(xk, wbuf[2 * slot + 1]), dg, du)
        return carry

    lax.fori_loop(0, FIRST, first_step, 0)

    cp(unperm, unperm_hbm, p_sem).start()
    wait(a_own)
    x_all.wait_recv()
    cls_recv = xa[recv, pl.ds(d_model, 128)].astype(F32)
    low_g, low_u = low_rank(recv, 0, n_all)
    pg[recv, :] = masked_bf16(low_g, cls_recv, 0)
    pu[recv, :] = masked_bf16(low_u, cls_recv, 0)
    pd[...] = jnp.zeros_like(pd)

    def add_low(tile, ad_slot):
        cols = tile_cols(tile)
        low_kept = dot_t(h[kept, cols], adbuf[ad_slot, hot_cols, :])
        low_recv = dot_t(h[recv, cols], adbuf[ad_slot])
        pd[kept, hot_cols] += low_kept
        pd[recv, :] += low_recv

    def recv_tile(tile, slot, between):
        xr = xa[recv, pl.ds(0, d_model)]
        dg, du = delta(pg[recv, :], bbuf[slot, 0]), delta(pu[recv, :], bbuf[slot, 1])
        g, u = dot(xr, wbuf[2 * slot]), dot(xr, wbuf[2 * slot + 1])
        between()
        h[recv, tile_cols(tile)] = act(g, u, dg, du)

    def all_tile(tile, slot, between):
        xx = xa[:, pl.ds(0, d_model)]
        g, u = dot(xx, wbuf[2 * slot]), dot(xx, wbuf[2 * slot + 1])
        dgk = delta(pg[kept, hot_cols], bbuf[slot, 0, hot_cols, :])
        dgr = delta(pg[recv, :], bbuf[slot, 0])
        duk = delta(pu[kept, hot_cols], bbuf[slot, 1, hot_cols, :])
        dur = delta(pu[recv, :], bbuf[slot, 1])
        between()
        h[kept, tile_cols(tile)] = act(g[:half], u[:half], dgk, duk)
        h[recv, tile_cols(tile)] = act(g[half:], u[half:], dgr, dur)

    wait(gu_extra(FIRST - 1, (FIRST - 1) % 3, 0))
    recv_tile(FIRST - 1, (FIRST - 1) % 3, lambda: None)

    def second_step(p, carry):
        s = 2 * p + 1
        wait(gu_full(FIRST + p, s))
        start(gu_full(FIRST + p + 1, s + 2))

        @pl.when(p == 1)
        def _():
            start(down_copies(0, (0, 1, 2)))

        all_tile(FIRST + p, ring(s), lambda: add_low(jnp.where(p == 0, FIRST - 1, p - 1), lax.rem(s + 3, 4)))
        wait(gu_full(p, s + 1))

        @pl.when(p + 2 < FIRST)
        def _():
            start(gu_full(p + 1, s + 3))

        @pl.when(p + 2 == FIRST)
        def _():
            start(down_copies(0, (3, 4)) + down_copies(1, (0, 1, 3, 4)))

        recv_tile(p, ring(s + 1), lambda: add_low(FIRST + p, lax.rem(s, 4)))
        return carry

    lax.fori_loop(0, FIRST - 1, second_step, 0)
    s_last = n_tiles - 1
    wait(gu_full(n_tiles - 1, s_last))
    start(down_copies(1, (2,)) + down_copies(2, (0, 3, 4)))
    all_tile(n_tiles - 1, (s_last + FIRST - 1) % 3, lambda: add_low(FIRST - 2, (s_last + 3) % 4))
    start(down_copies(2, (1, 2)))
    add_low(n_tiles - 1, (n_tiles - 1) % 4)

    pdm[kept, hot_cols] = masked_bf16(pd[kept, hot_cols], cls_kept, hot_group)
    pdm[recv, :] = masked_bf16(pd[recv, :], cls_recv, 0)

    def y_remote(n, d):
        to = lax.rem(me + d, group)
        return pltpu.make_async_remote_copy(
            src_ref=xy.at[n, pl.ds(pl.multiple_of(to * cap, cap), cap)], dst_ref=y_hbm.at[my_rows, tile_cols(n)],
            send_sem=s2.at[n], recv_sem=r2.at[n], device_id={"data": to}, device_id_type=MESH)

    def y_all(n):
        return pltpu.make_async_remote_copy(
            src_ref=xy.at[n, pl.ds(0, others)], dst_ref=y_hbm.at[pl.ds(half, others), tile_cols(n)],
            send_sem=s2.at[n], recv_sem=r2.at[n], device_id={"data": lax.rem(me + 1, group)}, device_id_type=MESH)

    def y_local(n):
        return [cp(xy.at[n, recv], y_hbm.at[kept, tile_cols(n)], y_sem.at[n, 0])]

    def y_self(n):
        return [cp(xy.at[n, my_block], y_hbm.at[my_rows, tile_cols(n)], y_sem.at[n, 1])]

    def rows_out(n, rows, low):
        y = low
        for i, (k, size) in enumerate(k_parts):
            y = dot(h[rows, pl.ds(k, size)], wbuf[down_half(n, i), pl.ds(0, size), :]) + y
        return (xa[rows, tile_cols(n)].astype(F32) + y).astype(BF16)

    def down_recv(n):
        slot, part = down_b(n)
        xy[n, kept, :] = rows_out(n, recv, delta(pdm[recv, :], bbuf[slot, part]).astype(F32))

    def down_kept(n):
        slot, part = down_b(n)
        xy[n, recv, :] = rows_out(n, kept, delta(pdm[kept, hot_cols], bbuf[slot, part, hot_cols, :]).astype(F32))

    def send_back(n):
        for d in range(1, group):
            y_remote(n, d).start()
        start(y_self(n))

    def down_step(n, carry):
        wait(down_copies(n))

        @pl.when(n > 0)
        def _():
            start(down_copies(n + 2))

        down_recv(n)
        down_kept(n)
        send_back(n)
        start(y_local(n))
        return carry

    early = d_tiles - 3
    lax.fori_loop(0, early, down_step, 0)
    start(down_copies(d_tiles - 1))

    def late_recv(n, carry):
        wait(down_copies(n))
        down_recv(n)
        send_back(n)
        return carry

    def late_kept(n, carry):
        down_kept(n)
        start(y_local(n))
        return carry

    lax.fori_loop(early, d_tiles, late_recv, 0)
    lax.fori_loop(early, d_tiles, late_kept, 0)

    x_all.wait_send()
    cp(unperm, unperm_hbm, p_sem).wait()
    for n in range(d_tiles):
        wait(y_self(n) + y_local(n))
        y_all(n).wait_send()
        y_all(n).wait_recv()


def place_kernel(y_hbm, unperm_hbm, out_hbm, y, unperm, out, y_sem, p_sem, o_sem):
    tiles = y.shape[0]

    def y_copy(n):
        return pltpu.make_async_copy(y_hbm.at[:, pl.ds(n * TN, TN)], y.at[n], y_sem.at[n])

    def o_copy(n):
        return pltpu.make_async_copy(out.at[n], out_hbm.at[:, pl.ds(n * TN, TN)], o_sem.at[n])

    p_copy = pltpu.make_async_copy(unperm_hbm, unperm, p_sem)
    p_copy.start()
    for n in range(tiles):
        y_copy(n).start()
    p_copy.wait()
    for group in ((0,), (1, 2), tuple(range(3, tiles))):
        for n in group:
            y_copy(n).wait()
        for n in group:
            out[n] = dot(unperm[...], y[n]).astype(BF16)
        for n in group:
            o_copy(n).start()
    for n in range(tiles):
        o_copy(n).wait()


def solution(mesh):
    group = mesh.shape["data"]
    token_spec = P(("replica", "data"), None)
    store_spec = P("data", None, None)
    full_mat = P(None, None)
    full_set = P(None, None, None)
    in_specs = (token_spec, P(("replica", "data")), full_mat, full_mat, full_mat) + (store_spec,) * 6 + (P(None),) + (full_set,) * 6

    def device_step(x, adapter_id, w_gate, w_up, w_down, a_gate, b_gate, a_up, b_up, a_down, b_down, hot_ids, hot_a_gate, hot_b_gate, hot_a_up, hot_b_up, hot_a_down, hot_b_down):
        tokens, d_model = x.shape
        d_ff = w_gate.shape[1]
        n_local, _, rank = a_gate.shape
        n_hot = hot_ids.shape[0]
        cap = tokens // (2 * group)
        half = group * cap
        n_all = (n_local + n_hot) * rank
        d_tiles = d_model // TN

        def a_t(a):
            return jnp.swapaxes(a, 1, 2).reshape(a.shape[0] * rank, a.shape[1])

        def b_flat(b):
            return b.reshape(b.shape[0] * rank, b.shape[2])

        hbm = pl.BlockSpec(memory_space=pl.ANY)
        kernel = functools.partial(mlp_kernel, group, n_local, n_hot, rank, LORA_ALPHA / rank)
        y, unperm = pl.pallas_call(
            kernel,
            out_shape=(jax.ShapeDtypeStruct(x.shape, x.dtype), jax.ShapeDtypeStruct((tokens, tokens), BF16)),
            in_specs=[hbm] * 18,
            out_specs=(hbm, hbm),
            scratch_shapes=[
                pltpu.SMEM((n_hot,), jnp.int32),
                pltpu.VMEM((1, tokens), jnp.int32),
                pltpu.VMEM((d_tiles, tokens, TN), BF16),
                pltpu.VMEM((half, d_model + 128), BF16),
                pltpu.VMEM((tokens, d_model + 128), BF16),
                pltpu.VMEM((tokens, d_ff), BF16),
                pltpu.VMEM((tokens, n_all), BF16),
                pltpu.VMEM((tokens, n_all), BF16),
                pltpu.VMEM((tokens, n_all), F32),
                pltpu.VMEM((tokens, n_all), BF16),
                pltpu.VMEM((9, d_model, TN), BF16),
                pltpu.VMEM((3, 2, n_all, TN), BF16),
                pltpu.VMEM((4, n_all, TN), BF16),
                pltpu.VMEM((tokens, tokens), BF16),
                pltpu.SemaphoreType.DMA((2,)),
                pltpu.SemaphoreType.DMA((d_tiles,)),
                pltpu.SemaphoreType.DMA((4, d_tiles)),
                pltpu.SemaphoreType.DMA((3, 6)),
                pltpu.SemaphoreType.DMA((4, 2)),
                pltpu.SemaphoreType.DMA((3, 5)),
                pltpu.SemaphoreType.DMA((d_tiles, 2)),
                pltpu.SemaphoreType.DMA,
                pltpu.SemaphoreType.DMA,
                pltpu.SemaphoreType.DMA,
                pltpu.SemaphoreType.DMA((d_tiles,)),
                pltpu.SemaphoreType.DMA((d_tiles,)),
            ],
            compiler_params=pltpu.CompilerParams(
                collective_id=0, has_side_effects=True, vmem_limit_bytes=67043328),
        )(hot_ids, adapter_id.reshape(1, tokens), x, w_gate, w_up, w_down,
          a_t(a_gate), b_flat(b_gate), a_t(a_up), b_flat(b_up), a_t(a_down), b_flat(b_down),
          a_t(hot_a_gate), b_flat(hot_b_gate), a_t(hot_a_up), b_flat(hot_b_up), a_t(hot_a_down), b_flat(hot_b_down))
        return pl.pallas_call(
            place_kernel,
            out_shape=jax.ShapeDtypeStruct(x.shape, x.dtype),
            in_specs=[hbm] * 2,
            out_specs=hbm,
            scratch_shapes=[
                pltpu.VMEM((d_tiles, tokens, TN), BF16),
                pltpu.VMEM((tokens, tokens), BF16),
                pltpu.VMEM((d_tiles, tokens, TN), BF16),
                pltpu.SemaphoreType.DMA((d_tiles,)),
                pltpu.SemaphoreType.DMA,
                pltpu.SemaphoreType.DMA((d_tiles,)),
            ],
        )(y, unperm)

    return jax.shard_map(device_step, mesh=mesh, in_specs=in_specs, out_specs=token_spec, check_vma=False)
```

```python
import functools

import jax
import jax.numpy as jnp
from jax import lax
from jax.experimental import pallas as pl
from jax.experimental.pallas import tpu as pltpu
from jax.sharding import PartitionSpec as P

LORA_ALPHA = 32
MESH = pl.DeviceIdType.MESH
F32 = jnp.float32
BF16 = jnp.bfloat16

TN = 512
FIRST = 9


def dot(a, b):
    return jnp.dot(a, b, preferred_element_type=F32)


def dot_t(a, b):
    return lax.dot_general(a, b, (((1,), (1,)), ((), ())), preferred_element_type=F32)


def earlier(tokens):
    row = lax.broadcasted_iota(jnp.int32, (tokens, tokens), 0)
    return (row < lax.broadcasted_iota(jnp.int32, (tokens, tokens), 1)).astype(BF16)


def positions(ids, hot_ids, before, n_hot, group, n_local, cap):
    tokens = ids.shape[1]
    kept = tokens - group * cap
    is_hot = ids < 0
    hot_idx = jnp.zeros_like(ids)
    for j in range(n_hot):
        match = ids == hot_ids[j]
        is_hot = is_hot | match
        hot_idx = jnp.where(match, j, hot_idx)
    owner = jnp.where(is_hot, group, ids // n_local)
    local = ids - (ids // n_local) * n_local
    cls = jnp.where(is_hot, n_local + hot_idx, local)
    rows = 2 * group
    kind = lax.broadcasted_iota(jnp.int32, (rows, tokens), 0)
    member = (kind == jnp.broadcast_to(owner, (rows, tokens))).astype(F32)
    cum = dot(member.astype(BF16), before)
    rank = jnp.sum(member * cum, axis=0, keepdims=True)
    counts = jnp.sum(member, axis=1, keepdims=True)
    sub = lax.broadcasted_iota(jnp.int32, (rows, 1), 0)
    holes = jnp.where(sub < group, cap - counts, 0.0)
    lower = lax.broadcasted_iota(jnp.int32, (rows, rows), 1) < lax.broadcasted_iota(jnp.int32, (rows, rows), 0)
    hole_start = dot(lower.astype(BF16), jnp.broadcast_to(holes, (rows, 128)).astype(BF16))[:, 0:1]
    spill = jnp.broadcast_to(rank - kept, (rows, tokens))
    takes = (spill >= hole_start) & (spill < hole_start + holes)
    base = kept + cap * sub.astype(F32) + counts - hole_start
    filled = jnp.sum(jnp.where(takes, base + spill, 0.0), axis=0, keepdims=True)
    own = kept + cap * owner.astype(F32) + rank
    pos = jnp.where(is_hot, jnp.where(rank < kept, rank, filled), own)
    return pos, cls.astype(F32)


def masked(low, cls, first_group, rank):
    per = 128 // rank
    lane = lax.broadcasted_iota(jnp.int32, (low.shape[0], 128), 1) // rank
    parts = []
    for k in range(low.shape[1] // 128):
        here = (lane + per * (first_group + k)).astype(F32) == cls
        parts.append(jnp.where(here, low[:, k * 128:(k + 1) * 128], 0.0).astype(BF16))
    return jnp.concatenate(parts, axis=1)


def mlp_kernel(group, n_local, n_hot, rank, scale,
               hot_hbm, ids_hbm, x_hbm, wg_hbm, wu_hbm, wd_hbm,
               ag_hbm, bg_hbm, au_hbm, bu_hbm, ad_hbm, bd_hbm,
               hag_hbm, hbg_hbm, hau_hbm, hbu_hbm, had_hbm, hbd_hbm,
               y_hbm, unperm_hbm,
               hot_ids, ids, xy, xsend, xa, h, pg, pu, pd, pdm, wbuf, bbuf, adbuf, unperm,
               id_sem, x_sem, at_sem, w_sem, ad_sem, d_sem, y_sem, p_sem, s1, r1, s2, r2):
    me = lax.axis_index("data")
    tokens, d_model = x_hbm.shape
    d_ff = wg_hbm.shape[1]
    cap = tokens // (2 * group)
    half = group * cap
    n_own = n_local * rank
    n_hr = n_hot * rank
    n_all = n_own + n_hr
    n_tiles = d_ff // TN
    d_tiles = d_model // TN
    kept = pl.ds(0, half)
    recv = pl.ds(half, half)
    own_cols = pl.ds(0, n_own)
    hot_cols = pl.ds(n_own, n_hr)
    hot_group = n_own // 128
    k_parts = [(k, min(d_model, d_ff - k)) for k in range(0, d_ff, d_model)]
    pairs = FIRST - 2
    assert len(k_parts) == 3 and n_tiles == FIRST + pairs and FIRST % 3 == 0

    def cp(src, dst, sem):
        return pltpu.make_async_copy(src, dst, sem)

    def tile_cols(tile):
        return pl.ds(tile * TN if isinstance(tile, int) else pl.multiple_of(tile * TN, TN), TN)

    def gu_base(tile, slot):
        cols = tile_cols(tile)
        return [
            cp(wg_hbm.at[:, cols], wbuf.at[2 * slot], w_sem.at[slot, 0]),
            cp(wu_hbm.at[:, cols], wbuf.at[2 * slot + 1], w_sem.at[slot, 1]),
            cp(hbg_hbm.at[:, cols], bbuf.at[slot, 0, hot_cols], w_sem.at[slot, 2]),
            cp(hbu_hbm.at[:, cols], bbuf.at[slot, 1, hot_cols], w_sem.at[slot, 3]),
        ]

    def gu_extra(tile, slot, ad_slot):
        cols = tile_cols(tile)
        return [
            cp(bg_hbm.at[:, cols], bbuf.at[slot, 0, own_cols], w_sem.at[slot, 4]),
            cp(bu_hbm.at[:, cols], bbuf.at[slot, 1, own_cols], w_sem.at[slot, 5]),
            cp(ad_hbm.at[:, cols], adbuf.at[ad_slot, own_cols], ad_sem.at[ad_slot, 0]),
            cp(had_hbm.at[:, cols], adbuf.at[ad_slot, hot_cols], ad_sem.at[ad_slot, 1]),
        ]

    def gu_full(tile, slot, ad_slot):
        return gu_base(tile, slot) + gu_extra(tile, slot, ad_slot)

    def a_view(i, c, first, size):
        index = i * d_tiles + c
        per = d_model // n_all
        return wbuf.at[6 + index // per, pl.ds((index % per) * n_all + first, size)]

    def a_copies(i, src, first, size, side):
        return [cp(src.at[:, pl.ds(c * TN, TN)], a_view(i, c, first, size), at_sem.at[2 * side + i, c]) for c in range(d_tiles)]

    def down_half(n, i):
        k = lax.rem(n, 3)
        return jnp.where(k == 0, 6 + i, 3 * (k - 1) + i)

    def down_b(n):
        k = lax.rem(n, 3)
        return k // 2, lax.rem(k, 2)

    def down_copies(n, pieces=(0, 1, 2, 3, 4)):
        cols = tile_cols(n)
        out = []
        for i in pieces:
            if i < 3:
                k, size = k_parts[i]
                src, dst = wd_hbm.at[pl.ds(k, size), cols], wbuf.at[down_half(n, i), pl.ds(0, size)]
            elif i == 3:
                src, dst = bd_hbm.at[:, cols], bbuf.at[down_b(n)[0], down_b(n)[1], own_cols]
            else:
                src, dst = hbd_hbm.at[:, cols], bbuf.at[down_b(n)[0], down_b(n)[1], hot_cols]
            out.append(cp(src, dst, d_sem.at[lax.rem(n, 3), i]))
        return out

    def start(copies):
        for c in copies:
            c.start()

    def wait(copies):
        for c in copies:
            c.wait()

    id_copies = [cp(ids_hbm, ids, id_sem.at[0]), cp(hot_hbm, hot_ids, id_sem.at[1])]
    x_copies = [cp(x_hbm.at[:, pl.ds(n * TN, TN)], xy.at[n], x_sem.at[n]) for n in range(d_tiles)]
    a_hot = a_copies(0, hag_hbm, n_own, n_hr, 0) + a_copies(1, hau_hbm, n_own, n_hr, 0)
    a_own = a_copies(0, ag_hbm, 0, n_own, 1) + a_copies(1, au_hbm, 0, n_own, 1)
    start(id_copies)
    start(x_copies)
    start(a_hot)
    start(gu_base(0, 0))
    start(gu_base(1, 1))

    barrier = pltpu.get_barrier_semaphore()
    for d in range(1, group):
        pl.semaphore_signal(barrier, inc=1, device_id={"data": lax.rem(me + d, group)}, device_id_type=MESH)

    before = earlier(tokens)
    wait(id_copies)
    pos, cls = positions(ids[...], hot_ids, before, n_hot, group, n_local, cap)
    place = jnp.broadcast_to(pos.astype(jnp.int32), (tokens, tokens))
    perm = (place == lax.broadcasted_iota(jnp.int32, (tokens, tokens), 0)).astype(BF16)
    cls_rows = dot_t(perm, jnp.broadcast_to(cls, (128, tokens)).astype(BF16)).astype(BF16)
    xsend[:, pl.ds(d_model, 128)] = cls_rows[half:]
    xa[kept, pl.ds(d_model, 128)] = cls_rows[:half]
    wait(x_copies)
    for n in range(d_tiles):
        xsend[:, pl.ds(n * TN, TN)] = dot(perm[half:], xy[n]).astype(BF16)

    pl.semaphore_wait(barrier, group - 1)
    my_block = pl.ds(pl.multiple_of(me * cap, cap), cap)
    my_rows = pl.ds(pl.multiple_of(half + me * cap, cap), cap)

    def x_remote(d):
        to = lax.rem(me + d, group)
        return pltpu.make_async_remote_copy(
            src_ref=xsend.at[pl.ds(pl.multiple_of(to * cap, cap), cap)], dst_ref=xa.at[my_rows],
            send_sem=s1, recv_sem=r1, device_id={"data": to}, device_id_type=MESH)

    others = (group - 1) * cap
    x_all = pltpu.make_async_remote_copy(
        src_ref=xsend.at[pl.ds(0, others)], dst_ref=xa.at[pl.ds(half, others)],
        send_sem=s1, recv_sem=r1, device_id={"data": lax.rem(me + 1, group)}, device_id_type=MESH)

    for d in range(1, group):
        x_remote(d).start()
    for n in range(d_tiles):
        xa[kept, pl.ds(n * TN, TN)] = dot(perm[:half], xy[n]).astype(BF16)
    wait(a_hot)
    xa[my_rows, :] = xsend[my_block, :]
    pos_col = jnp.transpose(jnp.broadcast_to(pos, (128, tokens)))[:, 0:1].astype(jnp.int32)
    unperm[...] = (pos_col == lax.broadcasted_iota(jnp.int32, (tokens, tokens), 1)).astype(BF16)

    def delta(low, b):
        return (scale * dot(low, b)).astype(BF16)

    def act(g, u, dg, du):
        g = g + dg.astype(F32)
        u = u + du.astype(F32)
        return (g * jax.nn.sigmoid(g) * u).astype(BF16)

    def low_rank(rows, first, size):
        low = [None, None]
        for c in range(d_tiles):
            for i in range(2):
                part = dot_t(xa[rows, pl.ds(c * TN, TN)], a_view(i, c, first, size)[...])
                low[i] = part if low[i] is None else low[i] + part
        return low

    def masked_bf16(low, cls, first_group):
        return masked(low.astype(BF16).astype(F32), cls, first_group, rank)

    cls_kept = xa[kept, pl.ds(d_model, 128)].astype(F32)
    low_g, low_u = low_rank(kept, n_own, n_hr)
    pg[kept, hot_cols] = masked_bf16(low_g, cls_kept, hot_group)
    pu[kept, hot_cols] = masked_bf16(low_u, cls_kept, hot_group)

    def first_step(s, carry):
        slot = lax.rem(s, 3)
        ahead = lax.rem(s + 2, 3)
        wait(gu_base(s, slot))

        @pl.when(s + 2 < FIRST)
        def _():
            start(gu_base(s + 2, ahead))

        @pl.when(s + 3 == FIRST)
        def _():
            start(gu_extra(FIRST - 1, ahead, 2))

        @pl.when(s + 2 >= FIRST)
        def _():
            start(gu_full(jnp.where(s + 2 == FIRST, FIRST, 0), ahead, jnp.where(s + 2 == FIRST, 3, 0)))

        @pl.when(s == 1)
        def _():
            start(a_own)

        xk = xa[kept, pl.ds(0, d_model)]
        dg = delta(pg[kept, hot_cols], bbuf[slot, 0, hot_cols, :])
        du = delta(pu[kept, hot_cols], bbuf[slot, 1, hot_cols, :])
        h[kept, tile_cols(s)] = act(dot(xk, wbuf[2 * slot]), dot(xk, wbuf[2 * slot + 1]), dg, du)
        return carry

    lax.fori_loop(0, FIRST, first_step, 0)

    cp(unperm, unperm_hbm, p_sem).start()
    wait(a_own)
    x_all.wait_recv()
    cls_recv = xa[recv, pl.ds(d_model, 128)].astype(F32)
    low_g, low_u = low_rank(recv, 0, n_all)
    pg[recv, :] = masked_bf16(low_g, cls_recv, 0)
    pu[recv, :] = masked_bf16(low_u, cls_recv, 0)
    pd[...] = jnp.zeros_like(pd)

    def add_low(tile, ad_slot):
        cols = tile_cols(tile)
        low_kept = dot_t(h[kept, cols], adbuf[ad_slot, hot_cols, :])
        low_recv = dot_t(h[recv, cols], adbuf[ad_slot])
        pd[kept, hot_cols] += low_kept
        pd[recv, :] += low_recv

    def recv_tile(tile, slot, between):
        xr = xa[recv, pl.ds(0, d_model)]
        dg, du = delta(pg[recv, :], bbuf[slot, 0]), delta(pu[recv, :], bbuf[slot, 1])
        g, u = dot(xr, wbuf[2 * slot]), dot(xr, wbuf[2 * slot + 1])
        between()
        h[recv, tile_cols(tile)] = act(g, u, dg, du)

    def all_tile(tile, slot, between):
        xx = xa[:, pl.ds(0, d_model)]
        g, u = dot(xx, wbuf[2 * slot]), dot(xx, wbuf[2 * slot + 1])
        dgk = delta(pg[kept, hot_cols], bbuf[slot, 0, hot_cols, :])
        dgr = delta(pg[recv, :], bbuf[slot, 0])
        duk = delta(pu[kept, hot_cols], bbuf[slot, 1, hot_cols, :])
        dur = delta(pu[recv, :], bbuf[slot, 1])
        between()
        h[kept, tile_cols(tile)] = act(g[:half], u[:half], dgk, duk)
        h[recv, tile_cols(tile)] = act(g[half:], u[half:], dgr, dur)

    wait(gu_extra(FIRST - 1, 2, 2))
    recv_tile(FIRST - 1, 2, lambda: None)

    def pair_copies(p):
        slot = 2 * lax.rem(p, 2)
        return gu_full(FIRST + p, slot, 3 + lax.rem(p, 2)) + gu_full(p, slot + 1, lax.rem(p, 3))

    def second_step(p, carry):
        slot = 2 * lax.rem(p, 2)
        wait(pair_copies(p))

        @pl.when(p + 1 < pairs)
        def _():
            start(pair_copies(p + 1))

        @pl.when(p + 1 == pairs)
        def _():
            start(gu_full(pairs, 2, pairs % 3))
            start(down_copies(0, (0, 1, 2)))

        all_tile(FIRST + p, slot, lambda: add_low(jnp.where(p == 0, FIRST - 1, p - 1), lax.rem(p + 2, 3)))
        recv_tile(p, slot + 1, lambda: add_low(FIRST + p, 3 + lax.rem(p, 2)))
        return carry

    lax.fori_loop(0, pairs, second_step, 0)
    wait(gu_full(pairs, 2, pairs % 3))
    start(down_copies(0, (3, 4)) + down_copies(1) + down_copies(2, (0, 3, 4)))
    recv_tile(pairs, 2, lambda: add_low(pairs - 1, (pairs - 1) % 3))
    start(down_copies(2, (1, 2)))
    add_low(pairs, pairs % 3)

    pdm[kept, hot_cols] = masked_bf16(pd[kept, hot_cols], cls_kept, hot_group)
    pdm[recv, :] = masked_bf16(pd[recv, :], cls_recv, 0)

    def y_remote(n, d):
        to = lax.rem(me + d, group)
        return pltpu.make_async_remote_copy(
            src_ref=xy.at[n, pl.ds(pl.multiple_of(to * cap, cap), cap)], dst_ref=y_hbm.at[my_rows, tile_cols(n)],
            send_sem=s2.at[n], recv_sem=r2.at[n], device_id={"data": to}, device_id_type=MESH)

    def y_all(n):
        return pltpu.make_async_remote_copy(
            src_ref=xy.at[n, pl.ds(0, others)], dst_ref=y_hbm.at[pl.ds(half, others), tile_cols(n)],
            send_sem=s2.at[n], recv_sem=r2.at[n], device_id={"data": lax.rem(me + 1, group)}, device_id_type=MESH)

    def y_local(n):
        return [cp(xy.at[n, recv], y_hbm.at[kept, tile_cols(n)], y_sem.at[n, 0])]

    def y_self(n):
        return [cp(xy.at[n, my_block], y_hbm.at[my_rows, tile_cols(n)], y_sem.at[n, 1])]

    def rows_out(n, rows, low):
        y = low
        for i, (k, size) in enumerate(k_parts):
            y = dot(h[rows, pl.ds(k, size)], wbuf[down_half(n, i), pl.ds(0, size), :]) + y
        return (xa[rows, tile_cols(n)].astype(F32) + y).astype(BF16)

    def down_recv(n):
        slot, part = down_b(n)
        xy[n, kept, :] = rows_out(n, recv, delta(pdm[recv, :], bbuf[slot, part]).astype(F32))

    def down_kept(n):
        slot, part = down_b(n)
        xy[n, recv, :] = rows_out(n, kept, delta(pdm[kept, hot_cols], bbuf[slot, part, hot_cols, :]).astype(F32))

    def send_back(n):
        for d in range(1, group):
            y_remote(n, d).start()
        start(y_self(n))

    def down_step(n, carry):
        wait(down_copies(n))

        @pl.when(n > 0)
        def _():
            start(down_copies(n + 2))

        down_recv(n)
        down_kept(n)
        send_back(n)
        start(y_local(n))
        return carry

    early = d_tiles - 3
    lax.fori_loop(0, early, down_step, 0)
    start(down_copies(d_tiles - 1))

    def late_recv(n, carry):
        wait(down_copies(n))
        down_recv(n)
        send_back(n)
        return carry

    def late_kept(n, carry):
        down_kept(n)
        start(y_local(n))
        return carry

    lax.fori_loop(early, d_tiles, late_recv, 0)
    lax.fori_loop(early, d_tiles, late_kept, 0)

    x_all.wait_send()
    cp(unperm, unperm_hbm, p_sem).wait()
    for n in range(d_tiles):
        wait(y_self(n) + y_local(n))
        y_all(n).wait_send()
        y_all(n).wait_recv()


def place_kernel(y_hbm, unperm_hbm, out_hbm, y, unperm, out, y_sem, p_sem, o_sem):
    tiles = y.shape[0]

    def y_copy(n):
        return pltpu.make_async_copy(y_hbm.at[:, pl.ds(n * TN, TN)], y.at[n], y_sem.at[n])

    def o_copy(n):
        return pltpu.make_async_copy(out.at[n], out_hbm.at[:, pl.ds(n * TN, TN)], o_sem.at[n])

    p_copy = pltpu.make_async_copy(unperm_hbm, unperm, p_sem)
    p_copy.start()
    for n in range(tiles):
        y_copy(n).start()
    p_copy.wait()
    for group in ((0,), (1, 2), tuple(range(3, tiles))):
        for n in group:
            y_copy(n).wait()
        for n in group:
            out[n] = dot(unperm[...], y[n]).astype(BF16)
        for n in group:
            o_copy(n).start()
    for n in range(tiles):
        o_copy(n).wait()


def solution(mesh):
    group = mesh.shape["data"]
    token_spec = P(("replica", "data"), None)
    store_spec = P("data", None, None)
    full_mat = P(None, None)
    full_set = P(None, None, None)
    in_specs = (token_spec, P(("replica", "data")), full_mat, full_mat, full_mat) + (store_spec,) * 6 + (P(None),) + (full_set,) * 6

    def device_step(x, adapter_id, w_gate, w_up, w_down, a_gate, b_gate, a_up, b_up, a_down, b_down, hot_ids, hot_a_gate, hot_b_gate, hot_a_up, hot_b_up, hot_a_down, hot_b_down):
        tokens, d_model = x.shape
        d_ff = w_gate.shape[1]
        n_local, _, rank = a_gate.shape
        n_hot = hot_ids.shape[0]
        cap = tokens // (2 * group)
        half = group * cap
        n_all = (n_local + n_hot) * rank
        d_tiles = d_model // TN

        def a_t(a):
            return jnp.swapaxes(a, 1, 2).reshape(a.shape[0] * rank, a.shape[1])

        def b_flat(b):
            return b.reshape(b.shape[0] * rank, b.shape[2])

        hbm = pl.BlockSpec(memory_space=pl.ANY)
        kernel = functools.partial(mlp_kernel, group, n_local, n_hot, rank, LORA_ALPHA / rank)
        y, unperm = pl.pallas_call(
            kernel,
            out_shape=(jax.ShapeDtypeStruct(x.shape, x.dtype), jax.ShapeDtypeStruct((tokens, tokens), BF16)),
            in_specs=[hbm] * 18,
            out_specs=(hbm, hbm),
            scratch_shapes=[
                pltpu.SMEM((n_hot,), jnp.int32),
                pltpu.VMEM((1, tokens), jnp.int32),
                pltpu.VMEM((d_tiles, tokens, TN), BF16),
                pltpu.VMEM((half, d_model + 128), BF16),
                pltpu.VMEM((tokens, d_model + 128), BF16),
                pltpu.VMEM((tokens, d_ff), BF16),
                pltpu.VMEM((tokens, n_all), BF16),
                pltpu.VMEM((tokens, n_all), BF16),
                pltpu.VMEM((tokens, n_all), F32),
                pltpu.VMEM((tokens, n_all), BF16),
                pltpu.VMEM((9, d_model, TN), BF16),
                pltpu.VMEM((4, 2, n_all, TN), BF16),
                pltpu.VMEM((5, n_all, TN), BF16),
                pltpu.VMEM((tokens, tokens), BF16),
                pltpu.SemaphoreType.DMA((2,)),
                pltpu.SemaphoreType.DMA((d_tiles,)),
                pltpu.SemaphoreType.DMA((4, d_tiles)),
                pltpu.SemaphoreType.DMA((4, 6)),
                pltpu.SemaphoreType.DMA((5, 2)),
                pltpu.SemaphoreType.DMA((3, 5)),
                pltpu.SemaphoreType.DMA((d_tiles, 2)),
                pltpu.SemaphoreType.DMA,
                pltpu.SemaphoreType.DMA,
                pltpu.SemaphoreType.DMA,
                pltpu.SemaphoreType.DMA((d_tiles,)),
                pltpu.SemaphoreType.DMA((d_tiles,)),
            ],
            compiler_params=pltpu.CompilerParams(
                collective_id=0, has_side_effects=True, vmem_limit_bytes=67043328),
        )(hot_ids, adapter_id.reshape(1, tokens), x, w_gate, w_up, w_down,
          a_t(a_gate), b_flat(b_gate), a_t(a_up), b_flat(b_up), a_t(a_down), b_flat(b_down),
          a_t(hot_a_gate), b_flat(hot_b_gate), a_t(hot_a_up), b_flat(hot_b_up), a_t(hot_a_down), b_flat(hot_b_down))
        return pl.pallas_call(
            place_kernel,
            out_shape=jax.ShapeDtypeStruct(x.shape, x.dtype),
            in_specs=[hbm] * 2,
            out_specs=hbm,
            scratch_shapes=[
                pltpu.VMEM((d_tiles, tokens, TN), BF16),
                pltpu.VMEM((tokens, tokens), BF16),
                pltpu.VMEM((d_tiles, tokens, TN), BF16),
                pltpu.SemaphoreType.DMA((d_tiles,)),
                pltpu.SemaphoreType.DMA,
                pltpu.SemaphoreType.DMA((d_tiles,)),
            ],
        )(y, unperm)

    return jax.shard_map(device_step, mesh=mesh, in_specs=in_specs, out_specs=token_spec, check_vma=False)
```

```python
import functools

import jax
import jax.numpy as jnp
from jax import lax
from jax.experimental import pallas as pl
from jax.experimental.pallas import tpu as pltpu
from jax.sharding import PartitionSpec as P

LORA_ALPHA = 32
MESH = pl.DeviceIdType.MESH
F32 = jnp.float32
BF16 = jnp.bfloat16

TN = 512
FIRST = 9


def dot(a, b):
    return jnp.dot(a, b, preferred_element_type=F32)


def dot_t(a, b):
    return lax.dot_general(a, b, (((1,), (1,)), ((), ())), preferred_element_type=F32)


def earlier(tokens):
    row = lax.broadcasted_iota(jnp.int32, (tokens, tokens), 0)
    return (row < lax.broadcasted_iota(jnp.int32, (tokens, tokens), 1)).astype(BF16)


def positions(ids, hot_ids, before, n_hot, group, n_local, cap):
    tokens = ids.shape[1]
    kept = tokens - group * cap
    is_hot = ids < 0
    hot_idx = jnp.zeros_like(ids)
    for j in range(n_hot):
        match = ids == hot_ids[j]
        is_hot = is_hot | match
        hot_idx = jnp.where(match, j, hot_idx)
    owner = jnp.where(is_hot, group, ids // n_local)
    local = ids - (ids // n_local) * n_local
    cls = jnp.where(is_hot, n_local + hot_idx, local)
    rows = 2 * group
    kind = lax.broadcasted_iota(jnp.int32, (rows, tokens), 0)
    member = (kind == jnp.broadcast_to(owner, (rows, tokens))).astype(F32)
    cum = dot(member.astype(BF16), before)
    rank = jnp.sum(member * cum, axis=0, keepdims=True)
    counts = jnp.sum(member, axis=1, keepdims=True)
    sub = lax.broadcasted_iota(jnp.int32, (rows, 1), 0)
    holes = jnp.where(sub < group, cap - counts, 0.0)
    lower = lax.broadcasted_iota(jnp.int32, (rows, rows), 1) < lax.broadcasted_iota(jnp.int32, (rows, rows), 0)
    hole_start = dot(lower.astype(BF16), jnp.broadcast_to(holes, (rows, 128)).astype(BF16))[:, 0:1]
    spill = jnp.broadcast_to(rank - kept, (rows, tokens))
    takes = (spill >= hole_start) & (spill < hole_start + holes)
    base = kept + cap * sub.astype(F32) + counts - hole_start
    filled = jnp.sum(jnp.where(takes, base + spill, 0.0), axis=0, keepdims=True)
    own = kept + cap * owner.astype(F32) + rank
    pos = jnp.where(is_hot, jnp.where(rank < kept, rank, filled), own)
    return pos, cls.astype(F32)


def masked(low, cls, first_group, rank):
    per = 128 // rank
    lane = lax.broadcasted_iota(jnp.int32, (low.shape[0], 128), 1) // rank
    parts = []
    for k in range(low.shape[1] // 128):
        here = (lane + per * (first_group + k)).astype(F32) == cls
        parts.append(jnp.where(here, low[:, k * 128:(k + 1) * 128], 0.0).astype(BF16))
    return jnp.concatenate(parts, axis=1)


def mlp_kernel(group, n_local, n_hot, rank, scale,
               hot_hbm, ids_hbm, x_hbm, wg_hbm, wu_hbm, wd_hbm,
               ag_hbm, bg_hbm, au_hbm, bu_hbm, ad_hbm, bd_hbm,
               hag_hbm, hbg_hbm, hau_hbm, hbu_hbm, had_hbm, hbd_hbm,
               y_hbm, unperm_hbm,
               hot_ids, ids, xy, xsend, xa, h, pg, pu, pd, pdm, wbuf, bbuf, adbuf, unperm,
               id_sem, x_sem, at_sem, w_sem, ad_sem, d_sem, y_sem, p_sem, s1, r1, s2, r2):
    me = lax.axis_index("data")
    tokens, d_model = x_hbm.shape
    d_ff = wg_hbm.shape[1]
    cap = tokens // (2 * group)
    half = group * cap
    n_own = n_local * rank
    n_hr = n_hot * rank
    n_all = n_own + n_hr
    n_tiles = d_ff // TN
    d_tiles = d_model // TN
    kept = pl.ds(0, half)
    recv = pl.ds(half, half)
    own_cols = pl.ds(0, n_own)
    hot_cols = pl.ds(n_own, n_hr)
    hot_group = n_own // 128
    k_parts = [(k, min(d_model, d_ff - k)) for k in range(0, d_ff, d_model)]
    pairs = FIRST - 2
    assert 2 * n_hr == d_model // 6 and n_own == 2 * n_hr
    assert len(k_parts) == 3 and n_tiles == FIRST + pairs and FIRST % 3 == 0

    def cp(src, dst, sem):
        return pltpu.make_async_copy(src, dst, sem)

    def tile_cols(tile):
        return pl.ds(tile * TN if isinstance(tile, int) else pl.multiple_of(tile * TN, TN), TN)

    def gu_base(tile, slot):
        cols = tile_cols(tile)
        return [
            cp(wg_hbm.at[:, cols], wbuf.at[2 * slot], w_sem.at[slot, 0]),
            cp(wu_hbm.at[:, cols], wbuf.at[2 * slot + 1], w_sem.at[slot, 0]),
            cp(hbg_hbm.at[:, cols], bbuf.at[slot, 0, hot_cols], w_sem.at[slot, 1]),
            cp(hbu_hbm.at[:, cols], bbuf.at[slot, 1, hot_cols], w_sem.at[slot, 1]),
        ]

    def gu_extra(tile, slot, ad_slot):
        cols = tile_cols(tile)
        return [
            cp(bg_hbm.at[:, cols], bbuf.at[slot, 0, own_cols], w_sem.at[slot, 2]),
            cp(bu_hbm.at[:, cols], bbuf.at[slot, 1, own_cols], w_sem.at[slot, 2]),
            cp(ad_hbm.at[:, cols], adbuf.at[ad_slot, own_cols], ad_sem.at[ad_slot]),
            cp(had_hbm.at[:, cols], adbuf.at[ad_slot, hot_cols], ad_sem.at[ad_slot]),
        ]

    def whole(ref, sem):
        return cp(ref, ref, sem)

    def base_done(slot):
        return [whole(wbuf.at[pl.ds(2 * slot, 2)], w_sem.at[slot, 0]), whole(bbuf.at[slot, :, hot_cols], w_sem.at[slot, 1])]

    def extra_done(slot, ad_slot):
        return [whole(bbuf.at[slot, :, own_cols], w_sem.at[slot, 2]), whole(adbuf.at[ad_slot], ad_sem.at[ad_slot])]

    def full_done(slot, ad_slot):
        return base_done(slot) + extra_done(slot, ad_slot)

    def gu_full(tile, slot, ad_slot):
        return gu_base(tile, slot) + gu_extra(tile, slot, ad_slot)

    def a_view(i, c, first, size):
        index = i * d_tiles + c
        per = d_model // n_all
        return wbuf.at[6 + index // per, pl.ds((index % per) * n_all + first, size)]

    def a_copies(i, src, first, size, side):
        return [cp(src.at[:, pl.ds(c * TN, TN)], a_view(i, c, first, size), at_sem.at[side]) for c in range(d_tiles)]

    def down_half(n, i):
        k = lax.rem(n, 3)
        return jnp.where(k == 0, 6 + i, 3 * (k - 1) + i)

    def down_b(n):
        k = lax.rem(n, 3)
        return k // 2, lax.rem(k, 2)

    def down_copies(n, pieces=(0, 1, 2, 3, 4)):
        cols = tile_cols(n)
        out = []
        for i in pieces:
            if i < 3:
                k, size = k_parts[i]
                src, dst = wd_hbm.at[pl.ds(k, size), cols], wbuf.at[down_half(n, i), pl.ds(0, size)]
            elif i == 3:
                src, dst = bd_hbm.at[:, cols], bbuf.at[down_b(n)[0], down_b(n)[1], own_cols]
            else:
                src, dst = hbd_hbm.at[:, cols], bbuf.at[down_b(n)[0], down_b(n)[1], hot_cols]
            out.append(cp(src, dst, d_sem.at[lax.rem(n, 3), i]))
        return out

    def start(copies):
        for c in copies:
            c.start()

    def wait(copies):
        for c in copies:
            c.wait()

    id_copies = [cp(ids_hbm, ids, id_sem.at[0]), cp(hot_hbm, hot_ids, id_sem.at[1])]
    x_copies = [cp(x_hbm.at[:, pl.ds(n * TN, TN)], xy.at[n], x_sem) for n in range(d_tiles)]
    a_hot = a_copies(0, hag_hbm, n_own, n_hr, 0) + a_copies(1, hau_hbm, n_own, n_hr, 0)
    a_own = a_copies(0, ag_hbm, 0, n_own, 1) + a_copies(1, au_hbm, 0, n_own, 1)
    start(id_copies)
    start(x_copies)
    start(a_hot)
    start(gu_base(0, 0))
    start(gu_base(1, 1))

    barrier = pltpu.get_barrier_semaphore()
    for d in range(1, group):
        pl.semaphore_signal(barrier, inc=1, device_id={"data": lax.rem(me + d, group)}, device_id_type=MESH)

    before = earlier(tokens)
    wait(id_copies)
    pos, cls = positions(ids[...], hot_ids, before, n_hot, group, n_local, cap)
    place = jnp.broadcast_to(pos.astype(jnp.int32), (tokens, tokens))
    perm = (place == lax.broadcasted_iota(jnp.int32, (tokens, tokens), 0)).astype(BF16)
    cls_rows = dot_t(perm, jnp.broadcast_to(cls, (128, tokens)).astype(BF16)).astype(BF16)
    xsend[:, pl.ds(d_model, 128)] = cls_rows[half:]
    xa[kept, pl.ds(d_model, 128)] = cls_rows[:half]
    wait([whole(xy, x_sem)])
    for n in range(d_tiles):
        xsend[:, pl.ds(n * TN, TN)] = dot(perm[half:], xy[n]).astype(BF16)

    pl.semaphore_wait(barrier, group - 1)
    my_block = pl.ds(pl.multiple_of(me * cap, cap), cap)
    my_rows = pl.ds(pl.multiple_of(half + me * cap, cap), cap)

    def x_remote(d):
        to = lax.rem(me + d, group)
        return pltpu.make_async_remote_copy(
            src_ref=xsend.at[pl.ds(pl.multiple_of(to * cap, cap), cap)], dst_ref=xa.at[my_rows],
            send_sem=s1, recv_sem=r1, device_id={"data": to}, device_id_type=MESH)

    others = (group - 1) * cap
    x_all = pltpu.make_async_remote_copy(
        src_ref=xsend.at[pl.ds(0, others)], dst_ref=xa.at[pl.ds(half, others)],
        send_sem=s1, recv_sem=r1, device_id={"data": lax.rem(me + 1, group)}, device_id_type=MESH)

    for d in range(1, group):
        x_remote(d).start()
    for n in range(d_tiles):
        xa[kept, pl.ds(n * TN, TN)] = dot(perm[:half], xy[n]).astype(BF16)
    wait([whole(wbuf.at[6], at_sem.at[0])])
    xa[my_rows, :] = xsend[my_block, :]
    pos_col = jnp.transpose(jnp.broadcast_to(pos, (128, tokens)))[:, 0:1].astype(jnp.int32)
    unperm[...] = (pos_col == lax.broadcasted_iota(jnp.int32, (tokens, tokens), 1)).astype(BF16)

    def delta(low, b):
        return (scale * dot(low, b)).astype(BF16)

    def act(g, u, dg, du):
        g = g + dg.astype(F32)
        u = u + du.astype(F32)
        return (g * jax.nn.sigmoid(g) * u).astype(BF16)

    def low_rank(rows, first, size):
        low = [None, None]
        for c in range(d_tiles):
            for i in range(2):
                part = dot_t(xa[rows, pl.ds(c * TN, TN)], a_view(i, c, first, size)[...])
                low[i] = part if low[i] is None else low[i] + part
        return low

    def masked_bf16(low, cls, first_group):
        return masked(low.astype(BF16).astype(F32), cls, first_group, rank)

    cls_kept = xa[kept, pl.ds(d_model, 128)].astype(F32)
    low_g, low_u = low_rank(kept, n_own, n_hr)
    pg[kept, hot_cols] = masked_bf16(low_g, cls_kept, hot_group)
    pu[kept, hot_cols] = masked_bf16(low_u, cls_kept, hot_group)

    def first_step(s, carry):
        slot = lax.rem(s, 3)
        ahead = lax.rem(s + 2, 3)
        wait(base_done(slot))

        @pl.when(s + 2 < FIRST)
        def _():
            start(gu_base(s + 2, ahead))

        @pl.when(s + 3 == FIRST)
        def _():
            start(gu_extra(FIRST - 1, ahead, 2))
            start(a_own)

        @pl.when(s + 2 >= FIRST)
        def _():
            start(gu_full(jnp.where(s + 2 == FIRST, FIRST, 0), ahead, jnp.where(s + 2 == FIRST, 3, 0)))

        xk = xa[kept, pl.ds(0, d_model)]
        dg = delta(pg[kept, hot_cols], bbuf[slot, 0, hot_cols, :])
        du = delta(pu[kept, hot_cols], bbuf[slot, 1, hot_cols, :])
        h[kept, tile_cols(s)] = act(dot(xk, wbuf[2 * slot]), dot(xk, wbuf[2 * slot + 1]), dg, du)
        return carry

    lax.fori_loop(0, FIRST, first_step, 0)

    cp(unperm, unperm_hbm, p_sem).start()
    wait([whole(wbuf.at[pl.ds(6, 2)], at_sem.at[1])])
    x_all.wait_recv()
    cls_recv = xa[recv, pl.ds(d_model, 128)].astype(F32)
    low_g, low_u = low_rank(recv, 0, n_all)
    pg[recv, :] = masked_bf16(low_g, cls_recv, 0)
    pu[recv, :] = masked_bf16(low_u, cls_recv, 0)
    pd[...] = jnp.zeros_like(pd)

    def add_low(tile, ad_slot):
        cols = tile_cols(tile)
        low_kept = dot_t(h[kept, cols], adbuf[ad_slot, hot_cols, :])
        low_recv = dot_t(h[recv, cols], adbuf[ad_slot])
        pd[kept, hot_cols] += low_kept
        pd[recv, :] += low_recv

    def recv_tile(tile, slot, between):
        xr = xa[recv, pl.ds(0, d_model)]
        dg, du = delta(pg[recv, :], bbuf[slot, 0]), delta(pu[recv, :], bbuf[slot, 1])
        g, u = dot(xr, wbuf[2 * slot]), dot(xr, wbuf[2 * slot + 1])
        between()
        h[recv, tile_cols(tile)] = act(g, u, dg, du)

    def all_tile(tile, slot, between):
        xx = xa[:, pl.ds(0, d_model)]
        g, u = dot(xx, wbuf[2 * slot]), dot(xx, wbuf[2 * slot + 1])
        dgk = delta(pg[kept, hot_cols], bbuf[slot, 0, hot_cols, :])
        dgr = delta(pg[recv, :], bbuf[slot, 0])
        duk = delta(pu[kept, hot_cols], bbuf[slot, 1, hot_cols, :])
        dur = delta(pu[recv, :], bbuf[slot, 1])
        between()
        h[kept, tile_cols(tile)] = act(g[:half], u[:half], dgk, duk)
        h[recv, tile_cols(tile)] = act(g[half:], u[half:], dgr, dur)

    wait(extra_done(2, 2))
    recv_tile(FIRST - 1, 2, lambda: None)

    def pair_copies(p):
        slot = 2 * lax.rem(p, 2)
        return gu_full(FIRST + p, slot, 3 + lax.rem(p, 2)) + gu_full(p, slot + 1, lax.rem(p, 3))

    def second_step(p, carry):
        slot = 2 * lax.rem(p, 2)
        wait(full_done(slot, 3 + lax.rem(p, 2)) + full_done(slot + 1, lax.rem(p, 3)))

        @pl.when(p + 1 < pairs)
        def _():
            start(pair_copies(p + 1))

        @pl.when(p + 1 == pairs)
        def _():
            start(gu_full(pairs, 2, pairs % 3))
            start(down_copies(0, (0, 1, 2)))

        all_tile(FIRST + p, slot, lambda: add_low(jnp.where(p == 0, FIRST - 1, p - 1), lax.rem(p + 2, 3)))
        recv_tile(p, slot + 1, lambda: add_low(FIRST + p, 3 + lax.rem(p, 2)))
        return carry

    lax.fori_loop(0, pairs, second_step, 0)
    wait(full_done(2, pairs % 3))
    start(down_copies(0, (3, 4)) + down_copies(1) + down_copies(2, (0, 3, 4)))
    recv_tile(pairs, 2, lambda: add_low(pairs - 1, (pairs - 1) % 3))
    start(down_copies(2, (1, 2)))
    add_low(pairs, pairs % 3)

    pdm[kept, hot_cols] = masked_bf16(pd[kept, hot_cols], cls_kept, hot_group)
    pdm[recv, :] = masked_bf16(pd[recv, :], cls_recv, 0)

    def y_remote(n, d):
        to = lax.rem(me + d, group)
        return pltpu.make_async_remote_copy(
            src_ref=xy.at[n, pl.ds(pl.multiple_of(to * cap, cap), cap)], dst_ref=y_hbm.at[my_rows, tile_cols(n)],
            send_sem=s2.at[n], recv_sem=r2.at[n], device_id={"data": to}, device_id_type=MESH)

    def y_all(n):
        return pltpu.make_async_remote_copy(
            src_ref=xy.at[n, pl.ds(0, others)], dst_ref=y_hbm.at[pl.ds(half, others), tile_cols(n)],
            send_sem=s2.at[n], recv_sem=r2.at[n], device_id={"data": lax.rem(me + 1, group)}, device_id_type=MESH)

    def y_local(n):
        return [cp(xy.at[n, recv], y_hbm.at[kept, tile_cols(n)], y_sem.at[n, 0])]

    def y_self(n):
        return [cp(xy.at[n, my_block], y_hbm.at[my_rows, tile_cols(n)], y_sem.at[n, 1])]

    def rows_out(n, rows, low):
        y = low
        for i, (k, size) in enumerate(k_parts):
            y = dot(h[rows, pl.ds(k, size)], wbuf[down_half(n, i), pl.ds(0, size), :]) + y
        return (xa[rows, tile_cols(n)].astype(F32) + y).astype(BF16)

    def down_recv(n):
        slot, part = down_b(n)
        xy[n, kept, :] = rows_out(n, recv, delta(pdm[recv, :], bbuf[slot, part]).astype(F32))

    def down_kept(n):
        slot, part = down_b(n)
        xy[n, recv, :] = rows_out(n, kept, delta(pdm[kept, hot_cols], bbuf[slot, part, hot_cols, :]).astype(F32))

    def send_back(n):
        for d in range(1, group):
            y_remote(n, d).start()
        start(y_self(n))

    def down_step(n, carry):
        wait(down_copies(n))

        @pl.when(n > 0)
        def _():
            start(down_copies(n + 2))

        down_recv(n)
        down_kept(n)
        send_back(n)
        start(y_local(n))
        return carry

    early = d_tiles - 3
    lax.fori_loop(0, early, down_step, 0)
    start(down_copies(d_tiles - 1))

    def late_recv(n, carry):
        wait(down_copies(n))
        down_recv(n)
        send_back(n)
        return carry

    lax.fori_loop(early, d_tiles, late_recv, 0)
    for n in range(early, d_tiles):
        down_kept(n)
    for n in range(early, d_tiles):
        start(y_local(n))

    x_all.wait_send()
    cp(unperm, unperm_hbm, p_sem).wait()
    for n in range(d_tiles):
        wait(y_self(n) + y_local(n))
        y_all(n).wait_send()
        y_all(n).wait_recv()


def place_kernel(y_hbm, unperm_hbm, out_hbm, y, unperm, out, y_sem, p_sem, o_sem):
    tiles = y.shape[0]

    def y_copy(n):
        return pltpu.make_async_copy(y_hbm.at[:, pl.ds(n * TN, TN)], y.at[n], y_sem.at[n])

    def o_copy(n):
        return pltpu.make_async_copy(out.at[n], out_hbm.at[:, pl.ds(n * TN, TN)], o_sem.at[n])

    p_copy = pltpu.make_async_copy(unperm_hbm, unperm, p_sem)
    p_copy.start()
    for n in range(tiles):
        y_copy(n).start()
    p_copy.wait()
    for group in ((0,), tuple(range(1, tiles - 2)), (tiles - 2, tiles - 1)):
        for n in group:
            y_copy(n).wait()
        for n in group:
            out[n] = dot(unperm[...], y[n]).astype(BF16)
        for n in group:
            o_copy(n).start()
    for n in range(tiles):
        o_copy(n).wait()


def solution(mesh):
    group = mesh.shape["data"]
    token_spec = P(("replica", "data"), None)
    store_spec = P("data", None, None)
    full_mat = P(None, None)
    full_set = P(None, None, None)
    in_specs = (token_spec, P(("replica", "data")), full_mat, full_mat, full_mat) + (store_spec,) * 6 + (P(None),) + (full_set,) * 6

    def device_step(x, adapter_id, w_gate, w_up, w_down, a_gate, b_gate, a_up, b_up, a_down, b_down, hot_ids, hot_a_gate, hot_b_gate, hot_a_up, hot_b_up, hot_a_down, hot_b_down):
        tokens, d_model = x.shape
        d_ff = w_gate.shape[1]
        n_local, _, rank = a_gate.shape
        n_hot = hot_ids.shape[0]
        cap = tokens // (2 * group)
        half = group * cap
        n_all = (n_local + n_hot) * rank
        d_tiles = d_model // TN

        def a_t(a):
            return jnp.swapaxes(a, 1, 2).reshape(a.shape[0] * rank, a.shape[1])

        def b_flat(b):
            return b.reshape(b.shape[0] * rank, b.shape[2])

        hbm = pl.BlockSpec(memory_space=pl.ANY)
        kernel = functools.partial(mlp_kernel, group, n_local, n_hot, rank, LORA_ALPHA / rank)
        y, unperm = pl.pallas_call(
            kernel,
            out_shape=(jax.ShapeDtypeStruct(x.shape, x.dtype), jax.ShapeDtypeStruct((tokens, tokens), BF16)),
            in_specs=[hbm] * 18,
            out_specs=(hbm, hbm),
            scratch_shapes=[
                pltpu.SMEM((n_hot,), jnp.int32),
                pltpu.VMEM((1, tokens), jnp.int32),
                pltpu.VMEM((d_tiles, tokens, TN), BF16),
                pltpu.VMEM((half, d_model + 128), BF16),
                pltpu.VMEM((tokens, d_model + 128), BF16),
                pltpu.VMEM((tokens, d_ff), BF16),
                pltpu.VMEM((tokens, n_all), BF16),
                pltpu.VMEM((tokens, n_all), BF16),
                pltpu.VMEM((tokens, n_all), F32),
                pltpu.VMEM((tokens, n_all), BF16),
                pltpu.VMEM((9, d_model, TN), BF16),
                pltpu.VMEM((4, 2, n_all, TN), BF16),
                pltpu.VMEM((5, n_all, TN), BF16),
                pltpu.VMEM((tokens, tokens), BF16),
                pltpu.SemaphoreType.DMA((2,)),
                pltpu.SemaphoreType.DMA,
                pltpu.SemaphoreType.DMA((2,)),
                pltpu.SemaphoreType.DMA((4, 3)),
                pltpu.SemaphoreType.DMA((5,)),
                pltpu.SemaphoreType.DMA((3, 5)),
                pltpu.SemaphoreType.DMA((d_tiles, 2)),
                pltpu.SemaphoreType.DMA,
                pltpu.SemaphoreType.DMA,
                pltpu.SemaphoreType.DMA,
                pltpu.SemaphoreType.DMA((d_tiles,)),
                pltpu.SemaphoreType.DMA((d_tiles,)),
            ],
            compiler_params=pltpu.CompilerParams(
                collective_id=0, has_side_effects=True, vmem_limit_bytes=67043328),
        )(hot_ids, adapter_id.reshape(1, tokens), x, w_gate, w_up, w_down,
          a_t(a_gate), b_flat(b_gate), a_t(a_up), b_flat(b_up), a_t(a_down), b_flat(b_down),
          a_t(hot_a_gate), b_flat(hot_b_gate), a_t(hot_a_up), b_flat(hot_b_up), a_t(hot_a_down), b_flat(hot_b_down))
        return pl.pallas_call(
            place_kernel,
            out_shape=jax.ShapeDtypeStruct(x.shape, x.dtype),
            in_specs=[hbm] * 2,
            out_specs=hbm,
            scratch_shapes=[
                pltpu.VMEM((d_tiles, tokens, TN), BF16),
                pltpu.VMEM((tokens, tokens), BF16),
                pltpu.VMEM((d_tiles, tokens, TN), BF16),
                pltpu.SemaphoreType.DMA((d_tiles,)),
                pltpu.SemaphoreType.DMA,
                pltpu.SemaphoreType.DMA((d_tiles,)),
            ],
        )(y, unperm)

    return jax.shard_map(device_step, mesh=mesh, in_specs=in_specs, out_specs=token_spec, check_vma=False)
```

```python
import functools

import jax
import jax.numpy as jnp
from jax import lax
from jax.experimental import pallas as pl
from jax.experimental.pallas import tpu as pltpu
from jax.sharding import PartitionSpec as P

LORA_ALPHA = 32
MESH = pl.DeviceIdType.MESH
F32 = jnp.float32
BF16 = jnp.bfloat16

TN = 512
FIRST = 9


def dot(a, b):
    return jnp.dot(a, b, preferred_element_type=F32)


def dot_t(a, b):
    return lax.dot_general(a, b, (((1,), (1,)), ((), ())), preferred_element_type=F32)


def earlier(tokens):
    row = lax.broadcasted_iota(jnp.int32, (tokens, tokens), 0)
    return (row < lax.broadcasted_iota(jnp.int32, (tokens, tokens), 1)).astype(BF16)


def positions(ids, hot_ids, before, n_hot, group, n_local, cap):
    tokens = ids.shape[1]
    kept = tokens - group * cap
    is_hot = ids < 0
    hot_idx = jnp.zeros_like(ids)
    for j in range(n_hot):
        match = ids == hot_ids[j]
        is_hot = is_hot | match
        hot_idx = jnp.where(match, j, hot_idx)
    owner = jnp.where(is_hot, group, ids // n_local)
    local = ids - (ids // n_local) * n_local
    cls = jnp.where(is_hot, n_local + hot_idx, local)
    rows = 2 * group
    kind = lax.broadcasted_iota(jnp.int32, (rows, tokens), 0)
    member = (kind == jnp.broadcast_to(owner, (rows, tokens))).astype(F32)
    cum = dot(member.astype(BF16), before)
    rank = jnp.sum(member * cum, axis=0, keepdims=True)
    counts = jnp.sum(member, axis=1, keepdims=True)
    sub = lax.broadcasted_iota(jnp.int32, (rows, 1), 0)
    holes = jnp.where(sub < group, cap - counts, 0.0)
    lower = lax.broadcasted_iota(jnp.int32, (rows, rows), 1) < lax.broadcasted_iota(jnp.int32, (rows, rows), 0)
    hole_start = dot(lower.astype(BF16), jnp.broadcast_to(holes, (rows, 128)).astype(BF16))[:, 0:1]
    spill = jnp.broadcast_to(rank - kept, (rows, tokens))
    takes = (spill >= hole_start) & (spill < hole_start + holes)
    base = kept + cap * sub.astype(F32) + counts - hole_start
    filled = jnp.sum(jnp.where(takes, base + spill, 0.0), axis=0, keepdims=True)
    own = kept + cap * owner.astype(F32) + rank
    pos = jnp.where(is_hot, jnp.where(rank < kept, rank, filled), own)
    return pos, cls.astype(F32)


def masked(low, cls, first_group, rank):
    per = 128 // rank
    lane = lax.broadcasted_iota(jnp.int32, (low.shape[0], 128), 1) // rank
    parts = []
    for k in range(low.shape[1] // 128):
        here = (lane + per * (first_group + k)).astype(F32) == cls
        parts.append(jnp.where(here, low[:, k * 128:(k + 1) * 128], 0.0).astype(BF16))
    return jnp.concatenate(parts, axis=1)


def mlp_kernel(group, n_local, n_hot, rank, scale,
               hot_hbm, ids_hbm, x_hbm, wg_hbm, wu_hbm, wd_hbm,
               ag_hbm, bg_hbm, au_hbm, bu_hbm, ad_hbm, bd_hbm,
               hag_hbm, hbg_hbm, hau_hbm, hbu_hbm, had_hbm, hbd_hbm,
               y_hbm, unperm_hbm,
               hot_ids, ids, xy, xsend, xa, h, pg, pu, pd, pdm, wbuf, bbuf, adbuf, unperm,
               id_sem, x_sem, self_sem, at_sem, w_sem, ad_sem, d_sem, y_sem, p_sem, s1, r1, s2, r2):
    me = lax.axis_index("data")
    tokens, d_model = x_hbm.shape
    d_ff = wg_hbm.shape[1]
    cap = tokens // (2 * group)
    half = group * cap
    n_own = n_local * rank
    n_hr = n_hot * rank
    n_all = n_own + n_hr
    n_tiles = d_ff // TN
    d_tiles = d_model // TN
    kept = pl.ds(0, half)
    recv = pl.ds(half, half)
    own_cols = pl.ds(0, n_own)
    hot_cols = pl.ds(n_own, n_hr)
    hot_group = n_own // 128
    k_parts = [(k, min(d_model, d_ff - k)) for k in range(0, d_ff, d_model)]
    pairs = FIRST - 2
    assert 2 * n_hr == d_model // 6 and n_own == 2 * n_hr
    assert len(k_parts) == 3 and n_tiles == FIRST + pairs and FIRST % 3 == 0

    def cp(src, dst, sem):
        return pltpu.make_async_copy(src, dst, sem)

    def tile_cols(tile):
        return pl.ds(tile * TN if isinstance(tile, int) else pl.multiple_of(tile * TN, TN), TN)

    def gu_base(tile, slot):
        cols = tile_cols(tile)
        return [
            cp(wg_hbm.at[:, cols], wbuf.at[2 * slot], w_sem.at[slot, 0]),
            cp(wu_hbm.at[:, cols], wbuf.at[2 * slot + 1], w_sem.at[slot, 0]),
            cp(hbg_hbm.at[:, cols], bbuf.at[slot, 0, hot_cols], w_sem.at[slot, 1]),
            cp(hbu_hbm.at[:, cols], bbuf.at[slot, 1, hot_cols], w_sem.at[slot, 1]),
        ]

    def gu_extra(tile, slot, ad_slot):
        cols = tile_cols(tile)
        return [
            cp(bg_hbm.at[:, cols], bbuf.at[slot, 0, own_cols], w_sem.at[slot, 2]),
            cp(bu_hbm.at[:, cols], bbuf.at[slot, 1, own_cols], w_sem.at[slot, 2]),
            cp(ad_hbm.at[:, cols], adbuf.at[ad_slot, own_cols], ad_sem.at[ad_slot]),
            cp(had_hbm.at[:, cols], adbuf.at[ad_slot, hot_cols], ad_sem.at[ad_slot]),
        ]

    def whole(ref, sem):
        return cp(ref, ref, sem)

    def base_done(slot):
        return [whole(wbuf.at[pl.ds(2 * slot, 2)], w_sem.at[slot, 0]), whole(bbuf.at[slot, :, hot_cols], w_sem.at[slot, 1])]

    def extra_done(slot, ad_slot):
        return [whole(bbuf.at[slot, :, own_cols], w_sem.at[slot, 2]), whole(adbuf.at[ad_slot], ad_sem.at[ad_slot])]

    def full_done(slot, ad_slot):
        return base_done(slot) + extra_done(slot, ad_slot)

    def gu_full(tile, slot, ad_slot):
        return gu_base(tile, slot) + gu_extra(tile, slot, ad_slot)

    def a_view(i, c, first, size):
        index = i * d_tiles + c
        per = d_model // n_all
        return wbuf.at[6 + index // per, pl.ds((index % per) * n_all + first, size)]

    def a_copies(i, src, first, size, side):
        return [cp(src.at[:, pl.ds(c * TN, TN)], a_view(i, c, first, size), at_sem.at[side]) for c in range(d_tiles)]

    def down_half(n, i):
        k = lax.rem(n, 3)
        return jnp.where(k == 0, 6 + i, 3 * (k - 1) + i)

    def down_b(n):
        k = lax.rem(n, 3)
        return k // 2, lax.rem(k, 2)

    def down_copies(n, pieces=(0, 1, 2, 3, 4)):
        cols = tile_cols(n)
        out = []
        for i in pieces:
            if i < 3:
                k, size = k_parts[i]
                src, dst = wd_hbm.at[pl.ds(k, size), cols], wbuf.at[down_half(n, i), pl.ds(0, size)]
            elif i == 3:
                src, dst = bd_hbm.at[:, cols], bbuf.at[down_b(n)[0], down_b(n)[1], own_cols]
            else:
                src, dst = hbd_hbm.at[:, cols], bbuf.at[down_b(n)[0], down_b(n)[1], hot_cols]
            out.append(cp(src, dst, d_sem.at[lax.rem(n, 3), i]))
        return out

    def start(copies):
        for c in copies:
            c.start()

    def wait(copies):
        for c in copies:
            c.wait()

    id_copies = [cp(ids_hbm, ids, id_sem.at[0]), cp(hot_hbm, hot_ids, id_sem.at[1])]
    x_copies = [cp(x_hbm.at[:, pl.ds(n * TN, TN)], xy.at[n], x_sem) for n in range(d_tiles)]
    a_hot = a_copies(0, hag_hbm, n_own, n_hr, 0) + a_copies(1, hau_hbm, n_own, n_hr, 0)
    a_own = a_copies(0, ag_hbm, 0, n_own, 1) + a_copies(1, au_hbm, 0, n_own, 1)
    start(id_copies)
    start(x_copies)
    start(a_hot)
    start(gu_base(0, 0))
    start(gu_base(1, 1))

    barrier = pltpu.get_barrier_semaphore()
    for d in range(1, group):
        pl.semaphore_signal(barrier, inc=1, device_id={"data": lax.rem(me + d, group)}, device_id_type=MESH)

    before = earlier(tokens)
    wait(id_copies)
    pos, cls = positions(ids[...], hot_ids, before, n_hot, group, n_local, cap)
    place = jnp.broadcast_to(pos.astype(jnp.int32), (tokens, tokens))
    perm = (place == lax.broadcasted_iota(jnp.int32, (tokens, tokens), 0)).astype(BF16)
    cls_rows = dot_t(perm, jnp.broadcast_to(cls, (128, tokens)).astype(BF16)).astype(BF16)
    xsend[:, pl.ds(d_model, 128)] = cls_rows[half:]
    xa[kept, pl.ds(d_model, 128)] = cls_rows[:half]
    wait([whole(xy, x_sem)])
    for n in range(d_tiles):
        xsend[:, pl.ds(n * TN, TN)] = dot(perm[half:], xy[n]).astype(BF16)

    pl.semaphore_wait(barrier, group - 1)
    my_block = pl.ds(pl.multiple_of(me * cap, cap), cap)
    my_rows = pl.ds(pl.multiple_of(half + me * cap, cap), cap)

    def x_remote(d):
        to = lax.rem(me + d, group)
        return pltpu.make_async_remote_copy(
            src_ref=xsend.at[pl.ds(pl.multiple_of(to * cap, cap), cap)], dst_ref=xa.at[my_rows],
            send_sem=s1, recv_sem=r1, device_id={"data": to}, device_id_type=MESH)

    others = (group - 1) * cap
    x_all = pltpu.make_async_remote_copy(
        src_ref=xsend.at[pl.ds(0, others)], dst_ref=xa.at[pl.ds(half, others)],
        send_sem=s1, recv_sem=r1, device_id={"data": lax.rem(me + 1, group)}, device_id_type=MESH)

    for d in range(1, group):
        x_remote(d).start()
    x_self = cp(xsend.at[my_block], xa.at[my_rows], self_sem)
    x_self.start()
    wait([whole(wbuf.at[6], at_sem.at[0])])
    for n in range(d_tiles):
        xa[kept, pl.ds(n * TN, TN)] = dot(perm[:half], xy[n]).astype(BF16)
    pos_col = jnp.transpose(jnp.broadcast_to(pos, (128, tokens)))[:, 0:1].astype(jnp.int32)
    unperm[...] = (pos_col == lax.broadcasted_iota(jnp.int32, (tokens, tokens), 1)).astype(BF16)

    def delta(low, b):
        return (scale * dot(low, b)).astype(BF16)

    def act(g, u, dg, du):
        g = g + dg.astype(F32)
        u = u + du.astype(F32)
        return (g * jax.nn.sigmoid(g) * u).astype(BF16)

    def low_rank(rows, first, size):
        low = [None, None]
        for c in range(d_tiles):
            for i in range(2):
                part = dot_t(xa[rows, pl.ds(c * TN, TN)], a_view(i, c, first, size)[...])
                low[i] = part if low[i] is None else low[i] + part
        return low

    def masked_bf16(low, cls, first_group):
        return masked(low.astype(BF16).astype(F32), cls, first_group, rank)

    cls_kept = xa[kept, pl.ds(d_model, 128)].astype(F32)
    low_g, low_u = low_rank(kept, n_own, n_hr)
    pg[kept, hot_cols] = masked_bf16(low_g, cls_kept, hot_group)
    pu[kept, hot_cols] = masked_bf16(low_u, cls_kept, hot_group)

    def first_step(s, carry):
        slot = lax.rem(s, 3)
        ahead = lax.rem(s + 2, 3)
        wait(base_done(slot))

        @pl.when(s + 2 < FIRST)
        def _():
            start(gu_base(s + 2, ahead))

        @pl.when(s + 3 == FIRST)
        def _():
            start(gu_extra(FIRST - 1, ahead, 2))
            start(a_own)

        @pl.when(s + 2 >= FIRST)
        def _():
            start(gu_full(jnp.where(s + 2 == FIRST, FIRST, 0), ahead, jnp.where(s + 2 == FIRST, 3, 0)))

        xk = xa[kept, pl.ds(0, d_model)]
        dg = delta(pg[kept, hot_cols], bbuf[slot, 0, hot_cols, :])
        du = delta(pu[kept, hot_cols], bbuf[slot, 1, hot_cols, :])
        h[kept, tile_cols(s)] = act(dot(xk, wbuf[2 * slot]), dot(xk, wbuf[2 * slot + 1]), dg, du)
        return carry

    lax.fori_loop(0, FIRST, first_step, 0)

    cp(unperm, unperm_hbm, p_sem).start()
    wait(extra_done(2, 2))
    x_self.wait()
    wait([whole(wbuf.at[pl.ds(6, 2)], at_sem.at[1])])
    x_all.wait_recv()
    pd[...] = jnp.zeros_like(pd)
    cls_recv = xa[recv, pl.ds(d_model, 128)].astype(F32)
    low_g, low_u = low_rank(recv, 0, n_all)
    pg[recv, :] = masked_bf16(low_g, cls_recv, 0)
    pu[recv, :] = masked_bf16(low_u, cls_recv, 0)

    def add_low(tile, ad_slot):
        cols = tile_cols(tile)
        low_kept = dot_t(h[kept, cols], adbuf[ad_slot, hot_cols, :])
        low_recv = dot_t(h[recv, cols], adbuf[ad_slot])
        pd[kept, hot_cols] += low_kept
        pd[recv, :] += low_recv

    def recv_tile(tile, slot, between):
        xr = xa[recv, pl.ds(0, d_model)]
        g, u = dot(xr, wbuf[2 * slot]), dot(xr, wbuf[2 * slot + 1])
        dg, du = delta(pg[recv, :], bbuf[slot, 0]), delta(pu[recv, :], bbuf[slot, 1])
        between()
        h[recv, tile_cols(tile)] = act(g, u, dg, du)

    def all_tile(tile, slot, between):
        xx = xa[:, pl.ds(0, d_model)]
        g, u = dot(xx, wbuf[2 * slot]), dot(xx, wbuf[2 * slot + 1])
        dgk = delta(pg[kept, hot_cols], bbuf[slot, 0, hot_cols, :])
        dgr = delta(pg[recv, :], bbuf[slot, 0])
        duk = delta(pu[kept, hot_cols], bbuf[slot, 1, hot_cols, :])
        dur = delta(pu[recv, :], bbuf[slot, 1])
        between()
        h[kept, tile_cols(tile)] = act(g[:half], u[:half], dgk, duk)
        h[recv, tile_cols(tile)] = act(g[half:], u[half:], dgr, dur)

    recv_tile(FIRST - 1, 2, lambda: None)

    def pair_copies(p):
        slot = 2 * lax.rem(p, 2)
        return gu_full(FIRST + p, slot, 3 + lax.rem(p, 2)) + gu_full(p, slot + 1, lax.rem(p, 3))

    def second_step(p, carry):
        slot = 2 * lax.rem(p, 2)
        wait(full_done(slot, 3 + lax.rem(p, 2)) + full_done(slot + 1, lax.rem(p, 3)))

        @pl.when(p + 1 < pairs)
        def _():
            start(pair_copies(p + 1))

        @pl.when(p + 1 == pairs)
        def _():
            start(gu_full(pairs, 2, pairs % 3))
            start(down_copies(0, (0, 1, 2)))

        all_tile(FIRST + p, slot, lambda: add_low(jnp.where(p == 0, FIRST - 1, p - 1), lax.rem(p + 2, 3)))
        recv_tile(p, slot + 1, lambda: add_low(FIRST + p, 3 + lax.rem(p, 2)))
        return carry

    lax.fori_loop(0, pairs, second_step, 0)
    wait(full_done(2, pairs % 3))
    start(down_copies(0, (3, 4)) + down_copies(1) + down_copies(2, (0, 3, 4)))
    recv_tile(pairs, 2, lambda: add_low(pairs - 1, (pairs - 1) % 3))
    start(down_copies(2, (1, 2)))
    add_low(pairs, pairs % 3)

    pdm[kept, hot_cols] = masked_bf16(pd[kept, hot_cols], cls_kept, hot_group)
    pdm[recv, :] = masked_bf16(pd[recv, :], cls_recv, 0)

    def y_remote(n, d):
        to = lax.rem(me + d, group)
        return pltpu.make_async_remote_copy(
            src_ref=xy.at[n, pl.ds(pl.multiple_of(to * cap, cap), cap)], dst_ref=y_hbm.at[my_rows, tile_cols(n)],
            send_sem=s2.at[n], recv_sem=r2.at[n], device_id={"data": to}, device_id_type=MESH)

    def y_all(n):
        return pltpu.make_async_remote_copy(
            src_ref=xy.at[n, pl.ds(0, others)], dst_ref=y_hbm.at[pl.ds(half, others), tile_cols(n)],
            send_sem=s2.at[n], recv_sem=r2.at[n], device_id={"data": lax.rem(me + 1, group)}, device_id_type=MESH)

    def y_local(n):
        return [cp(xy.at[n, recv], y_hbm.at[kept, tile_cols(n)], y_sem.at[n, 0])]

    def y_self(n):
        return [cp(xy.at[n, my_block], y_hbm.at[my_rows, tile_cols(n)], y_sem.at[n, 1])]

    def rows_out(n, rows, low):
        y = low
        for i, (k, size) in enumerate(k_parts):
            y = dot(h[rows, pl.ds(k, size)], wbuf[down_half(n, i), pl.ds(0, size), :]) + y
        return (xa[rows, tile_cols(n)].astype(F32) + y).astype(BF16)

    def down_recv(n):
        slot, part = down_b(n)
        xy[n, kept, :] = rows_out(n, recv, delta(pdm[recv, :], bbuf[slot, part]).astype(F32))

    def down_kept(n):
        slot, part = down_b(n)
        xy[n, recv, :] = rows_out(n, kept, delta(pdm[kept, hot_cols], bbuf[slot, part, hot_cols, :]).astype(F32))

    def send_back(n):
        for d in range(1, group):
            y_remote(n, d).start()
        start(y_self(n))

    def down_step(n, carry):
        wait(down_copies(n))

        @pl.when(n > 0)
        def _():
            start(down_copies(n + 2))

        down_recv(n)
        down_kept(n)
        send_back(n)
        start(y_local(n))
        return carry

    early = d_tiles - 3
    lax.fori_loop(0, early, down_step, 0)
    start(down_copies(d_tiles - 1))

    def late_recv(n, carry):
        wait(down_copies(n))
        down_recv(n)
        send_back(n)
        return carry

    lax.fori_loop(early, d_tiles, late_recv, 0)
    for n in range(early, d_tiles):
        down_kept(n)
    for n in range(early, d_tiles):
        start(y_local(n))

    x_all.wait_send()
    cp(unperm, unperm_hbm, p_sem).wait()
    for n in range(d_tiles):
        wait(y_self(n) + y_local(n))
        y_all(n).wait_send()
        y_all(n).wait_recv()


def place_kernel(y_hbm, unperm_hbm, out_hbm, y, unperm, out, y_sem, p_sem, o_sem):
    tiles = y.shape[0]

    def y_copy(n):
        return pltpu.make_async_copy(y_hbm.at[:, pl.ds(n * TN, TN)], y.at[n], y_sem.at[n])

    def o_copy(n):
        return pltpu.make_async_copy(out.at[n], out_hbm.at[:, pl.ds(n * TN, TN)], o_sem.at[n])

    p_copy = pltpu.make_async_copy(unperm_hbm, unperm, p_sem)
    p_copy.start()
    for n in range(tiles):
        y_copy(n).start()
    p_copy.wait()
    for group in ((0,), tuple(range(1, tiles - 2)), (tiles - 2, tiles - 1)):
        for n in group:
            y_copy(n).wait()
        for n in group:
            out[n] = dot(unperm[...], y[n]).astype(BF16)
        for n in group:
            o_copy(n).start()
    for n in range(tiles):
        o_copy(n).wait()


def solution(mesh):
    group = mesh.shape["data"]
    token_spec = P(("replica", "data"), None)
    store_spec = P("data", None, None)
    full_mat = P(None, None)
    full_set = P(None, None, None)
    in_specs = (token_spec, P(("replica", "data")), full_mat, full_mat, full_mat) + (store_spec,) * 6 + (P(None),) + (full_set,) * 6

    def device_step(x, adapter_id, w_gate, w_up, w_down, a_gate, b_gate, a_up, b_up, a_down, b_down, hot_ids, hot_a_gate, hot_b_gate, hot_a_up, hot_b_up, hot_a_down, hot_b_down):
        tokens, d_model = x.shape
        d_ff = w_gate.shape[1]
        n_local, _, rank = a_gate.shape
        n_hot = hot_ids.shape[0]
        cap = tokens // (2 * group)
        half = group * cap
        n_all = (n_local + n_hot) * rank
        d_tiles = d_model // TN

        def a_t(a):
            return jnp.swapaxes(a, 1, 2).reshape(a.shape[0] * rank, a.shape[1])

        def b_flat(b):
            return b.reshape(b.shape[0] * rank, b.shape[2])

        hbm = pl.BlockSpec(memory_space=pl.ANY)
        kernel = functools.partial(mlp_kernel, group, n_local, n_hot, rank, LORA_ALPHA / rank)
        y, unperm = pl.pallas_call(
            kernel,
            out_shape=(jax.ShapeDtypeStruct(x.shape, x.dtype), jax.ShapeDtypeStruct((tokens, tokens), BF16)),
            in_specs=[hbm] * 18,
            out_specs=(hbm, hbm),
            scratch_shapes=[
                pltpu.SMEM((n_hot,), jnp.int32),
                pltpu.VMEM((1, tokens), jnp.int32),
                pltpu.VMEM((d_tiles, tokens, TN), BF16),
                pltpu.VMEM((half, d_model + 128), BF16),
                pltpu.VMEM((tokens, d_model + 128), BF16),
                pltpu.VMEM((tokens, d_ff), BF16),
                pltpu.VMEM((tokens, n_all), BF16),
                pltpu.VMEM((tokens, n_all), BF16),
                pltpu.VMEM((tokens, n_all), F32),
                pltpu.VMEM((tokens, n_all), BF16),
                pltpu.VMEM((9, d_model, TN), BF16),
                pltpu.VMEM((4, 2, n_all, TN), BF16),
                pltpu.VMEM((5, n_all, TN), BF16),
                pltpu.VMEM((tokens, tokens), BF16),
                pltpu.SemaphoreType.DMA((2,)),
                pltpu.SemaphoreType.DMA,
                pltpu.SemaphoreType.DMA,
                pltpu.SemaphoreType.DMA((2,)),
                pltpu.SemaphoreType.DMA((4, 3)),
                pltpu.SemaphoreType.DMA((5,)),
                pltpu.SemaphoreType.DMA((3, 5)),
                pltpu.SemaphoreType.DMA((d_tiles, 2)),
                pltpu.SemaphoreType.DMA,
                pltpu.SemaphoreType.DMA,
                pltpu.SemaphoreType.DMA,
                pltpu.SemaphoreType.DMA((d_tiles,)),
                pltpu.SemaphoreType.DMA((d_tiles,)),
            ],
            compiler_params=pltpu.CompilerParams(
                collective_id=0, has_side_effects=True, vmem_limit_bytes=67043328),
        )(hot_ids, adapter_id.reshape(1, tokens), x, w_gate, w_up, w_down,
          a_t(a_gate), b_flat(b_gate), a_t(a_up), b_flat(b_up), a_t(a_down), b_flat(b_down),
          a_t(hot_a_gate), b_flat(hot_b_gate), a_t(hot_a_up), b_flat(hot_b_up), a_t(hot_a_down), b_flat(hot_b_down))
        return pl.pallas_call(
            place_kernel,
            out_shape=jax.ShapeDtypeStruct(x.shape, x.dtype),
            in_specs=[hbm] * 2,
            out_specs=hbm,
            scratch_shapes=[
                pltpu.VMEM((d_tiles, tokens, TN), BF16),
                pltpu.VMEM((tokens, tokens), BF16),
                pltpu.VMEM((d_tiles, tokens, TN), BF16),
                pltpu.SemaphoreType.DMA((d_tiles,)),
                pltpu.SemaphoreType.DMA,
                pltpu.SemaphoreType.DMA((d_tiles,)),
            ],
        )(y, unperm)

    return jax.shard_map(device_step, mesh=mesh, in_specs=in_specs, out_specs=token_spec, check_vma=False)
```
